512 devices in a mesh: ens: 2 (over y), lon: 32 (over z), lat: 4 (over x), ch: 2 (over core).
Axes of the slice: x: 4, y: 2, z: 32, core: 2. Of those that a mesh axis runs over, the one named last changes fastest.
The devices are a block of a 4x16x32 slice.
Arguments:
- input_field: bfloat16 [512, 1024, 128], P(('ens', 'lat', 'ch'), 'lon'), parts along dimension 0, may hold values from -6 to 6
- encoder_filter: bfloat16 [256, 4, 5], P(('lat', 'ch')), may hold values from -2.6875 to 2.6875
- row_owner: int32 [512], P(('ens', 'lat', 'ch')), parts along dimension 0, may hold values from 0 to 127, as said below
- encoder_weight: bfloat16 [512, 256], replicated, may hold values from -0.25 to 0.25
- disco_basis: bfloat16 [128, 4, 3, 17], P(('lat', 'ch')), may hold values from -1.5 to 1.5
- row_widths: int32 [128], P(('lat', 'ch')), may hold values from 1 to 8, as said below
- block_weights: bfloat16 [2, 1024, 256], replicated, may hold values from -0.1875 to 0.1875
- cotangent: bfloat16 [256, 512, 256], P(('ens', 'lat', 'ch'), 'lon'), parts along dimension 0, may hold values from -6 to 6
Outputs:
- state_out: bfloat16 [256, 512, 256], P(('ens', 'lat', 'ch'), 'lon'), parts along dimension 0
- latent_grad: bfloat16 [256, 512, 256], P(('ens', 'lat', 'ch'), 'lon'), parts along dimension 0
- block_grads: float32 [4, 1024, 256], P('ens', None, 'ch'), parts along dimension 0
- encoder_grad: float32 [1024, 256], P('ens', 'ch'), parts along dimension 0
The draws below stay inside these ranges and needn't reach their ends.
There are 2 independent parts, one for each index of `ens`. The reference program is written for one: setup_inputs(seed, part) draws one part's arguments, and reference() takes and returns one part's arrays. A program takes and returns all parts, laid end to end along the dimension named above; an argument that names none is the same for every part. Nothing has to cross between parts.
Inputs may be any that keep to these rules, and one draw needn't show every extreme that they name: `row_owner`: input row p feeds latent row (p - 1) // 2, p // 2 or (p + 1) // 2, and every latent row is fed by 1 to 3 input rows. `row_widths`: the first and last rows have 8.
All inputs are finite; a program needn't handle non-finite values.
Results may differ from the reference program's by a relative error of at most 0.014.
Values may be sent and summed in bfloat16 or wider, within the bound.
No kernel may reach another device: no remote copies, remote signals or barrier semaphores. Data moves between devices by JAX's collectives and lax.ppermute only.
A program may use at most 64 MiB of HBM per device.

```python
import math
import jax
import jax.numpy as jnp
from jax import lax

CHANNELS = 256
IN_CHANNELS = 128
BASIS = 4
REACH = 8
TAP_REACH = 2
BLOCKS = 2
ROWS_DEV = 16
NLAT = 128
NLON = 512
NLAT_IN = 256
NLON_IN = 1024


def draw_row_owner(key, part):
    key_moves = jax.random.fold_in(key, 11)
    position = jnp.arange(NLAT + 1, dtype=jnp.int32)
    stepping = jax.random.randint(key_moves, (NLAT + 1,), -1, 2, dtype=jnp.int32)
    drifts = jnp.where(position % 2 == 1, 0, stepping)
    at_edge = position % ROWS_DEV == 0
    drifts = jnp.where(at_edge, 0, drifts)
    starts = 2 * position + drifts
    input_rows = jnp.arange(2 * NLAT, dtype=jnp.int32)
    inside = (starts[None, 1:NLAT] <= input_rows[:, None]).astype(jnp.int32)
    owners = jnp.sum(inside, axis=1).astype(jnp.int32)
    band_rows = 2 * ROWS_DEV
    first_of_band = (input_rows % band_rows == 0) & (input_rows > 0)
    last_of_band = (input_rows % band_rows == band_rows - 1) & (input_rows < 2 * NLAT - 1)
    owners = jnp.where(first_of_band, owners - 1, owners)
    owners = jnp.where(last_of_band, owners + 1, owners)
    return owners.astype(jnp.int32)


def draw_row_widths(key, part):
    position = jnp.arange(NLAT, dtype=jnp.int32)
    distance = jnp.abs(2 * position + 1 - NLAT)
    jitter = jax.random.randint(jax.random.fold_in(key, 23), (NLAT,), 0, 2, dtype=jnp.int32)
    widths = 1 + jitter + (REACH - 2) * distance * distance // (NLAT * NLAT)
    widths = jnp.where((position == 0) | (position == NLAT - 1), REACH, widths)
    return jnp.clip(widths, 1, REACH).astype(jnp.int32)


def block_levels(own_key, extent, cuts, smallest, top_value):
    factor_of, own = 1.0, jax.random.fold_in(own_key, 6)
    for dim, shards_of in cuts:
        draws = jnp.exp(jax.random.uniform(jax.random.fold_in(own, dim), (shards_of,), jnp.float32, smallest / len(cuts), top_value / len(cuts)))
        factor_of = factor_of * jnp.repeat(draws, extent[dim] // shards_of).reshape([-1 if axis == dim else 1 for axis in range(len(extent))])
    return factor_of


def bell_draw(rng, dims, width, limit, shards=(), held_as=jnp.bfloat16):
    entries = width * jax.random.normal(rng, dims, jnp.float32)
    if shards:
        entries = entries * block_levels(rng, dims, shards, -0.22, 0.18)
    return jnp.clip(entries, -limit, limit).astype(held_as)


def setup_inputs(seed: int = 0, part: int = 0) -> dict:
    splits = jax.random.split(jax.random.key(seed), 9)
    part_keys = jax.random.split(jax.random.fold_in(splits[8], part), 9)
    return {
        "input_field": bell_draw(part_keys[0], (NLAT_IN, NLON_IN, IN_CHANNELS), 1.0, 6.0, ((0, 8), (1, 32))),
        "encoder_filter": bell_draw(splits[1], (NLAT_IN, BASIS, 2 * TAP_REACH + 1), 0.45, 2.6875, ((0, 8),)),
        "row_owner": draw_row_owner(jax.random.fold_in(jax.random.fold_in(splits[8], part), 71), part),
        "encoder_weight": bell_draw(splits[3], (BASIS * IN_CHANNELS, CHANNELS), (BASIS * IN_CHANNELS) ** -0.5, 0.25),
        "disco_basis": bell_draw(splits[4], (NLAT, BASIS, 3, 2 * REACH + 1), 0.25, 1.5, ((0, 8),)),
        "row_widths": draw_row_widths(jax.random.fold_in(splits[8], 71), part),
        "block_weights": bell_draw(splits[6], (BLOCKS, BASIS * CHANNELS, CHANNELS), (BASIS * CHANNELS) ** -0.5, 0.1875),
        "cotangent": bell_draw(part_keys[7], (NLAT, NLON, CHANNELS), 1.0, 6.0, ((0, 8), (1, 32))),
    }


def masked_basis(disco_basis, row_widths):
    offsets = jnp.abs(jnp.arange(2 * REACH + 1, dtype=jnp.int32) - REACH)
    keep = offsets[None, :] <= row_widths[:, None]
    values = disco_basis.astype(jnp.float32)
    return jnp.where(keep[:, None, None, :], values, jnp.zeros_like(values))

def apply_stencil(field, basis):
    padded = jnp.pad(field, ((1, 1), (0, 0), (0, 0)))
    padded = jnp.concatenate([padded[:, NLON - REACH:], padded, padded[:, :REACH]], axis=1)
    stacked = jnp.stack([padded[0:NLAT], padded[1:NLAT + 1], padded[2:NLAT + 2]], axis=0)
    result = jnp.zeros((NLAT, NLON, BASIS, CHANNELS), field.dtype)
    for shift_col in range(2 * REACH + 1):
        window = stacked[:, :, shift_col:shift_col + NLON, :]
        result = result + jnp.einsum('rijc,ikr->ijkc', window, basis[:, :, :, shift_col], precision=lax.Precision.HIGHEST)
    return result

def reference(input_field, encoder_filter, row_owner, encoder_weight, disco_basis, row_widths, block_weights, cotangent):
    field_in = input_field.astype(jnp.float32)
    wrapped = jnp.concatenate([field_in[:, NLON_IN - TAP_REACH:], field_in, field_in[:, :TAP_REACH]], axis=1)
    filter_values = encoder_filter.astype(jnp.float32)
    accumulated = jnp.zeros((NLAT_IN, NLON, BASIS, IN_CHANNELS), field_in.dtype)
    for tap_index in range(2 * TAP_REACH + 1):
        sampled = wrapped[:, tap_index:tap_index + NLON_IN:2, :]
        accumulated = accumulated + sampled[:, :, None, :] * filter_values[:, None, :, tap_index, None]
    filtered_input = accumulated.astype(jnp.bfloat16)
    regridded = jax.ops.segment_sum(filtered_input.astype(jnp.float32), row_owner, num_segments=NLAT)
    latent_input = regridded.astype(jnp.bfloat16).reshape(NLAT * NLON, BASIS * IN_CHANNELS)
    current = jnp.dot(latent_input, encoder_weight, preferred_element_type=jnp.float32).astype(jnp.bfloat16)
    current = current.reshape(NLAT, NLON, CHANNELS)
    basis = masked_basis(disco_basis, row_widths)
    saved = []
    for layer_index in range(BLOCKS):
        features = apply_stencil(current.astype(jnp.float32), basis).astype(jnp.bfloat16)
        features = features.reshape(NLAT * NLON, BASIS * CHANNELS)
        preact = jnp.dot(features, block_weights[layer_index], preferred_element_type=jnp.float32)
        current = (current.astype(jnp.float32) + jax.nn.silu(preact).reshape(NLAT, NLON, CHANNELS)).astype(jnp.bfloat16)
        saved.append((features, preact))
    state_out = current
    zero_field = jnp.zeros((NLAT, NLON, CHANNELS), jnp.float32)
    unused, pullback = jax.vjp(lambda field: apply_stencil(field, basis), zero_field)
    gradient = cotangent
    weight_terms = [None] * BLOCKS
    for layer_index in reversed(range(BLOCKS)):
        features, preact = saved[layer_index]
        sigma = jax.nn.sigmoid(preact)
        upstream = gradient.reshape(NLAT * NLON, CHANNELS).astype(jnp.float32)
        act_grad = (upstream * sigma * (1.0 + preact * (1.0 - sigma))).astype(jnp.bfloat16)
        weight_terms[layer_index] = jnp.dot(features.T, act_grad, preferred_element_type=jnp.float32)
        errors = jnp.dot(act_grad, block_weights[layer_index].T, preferred_element_type=jnp.float32).astype(jnp.bfloat16)
        errors = errors.reshape(NLAT, NLON, BASIS, CHANNELS)
        spread = pullback(errors.astype(jnp.float32))[0]
        gradient = (gradient.astype(jnp.float32) + spread).astype(jnp.bfloat16)
    normalizer = 1.0 / math.sqrt(NLAT * NLON)
    encoder_term = jnp.dot(latent_input.T, gradient.reshape(NLAT * NLON, CHANNELS), preferred_element_type=jnp.float32)
    block_grads = jnp.stack(weight_terms, axis=0) * normalizer
    return (state_out, gradient, block_grads, encoder_term * normalizer)
```

```python
import math

import jax
import jax.numpy as jnp
from jax import lax
from jax.sharding import PartitionSpec as P

REACH = 8
TAP_REACH = 2


def passed_along(value, axis, steps):
    count = lax.axis_size(axis)
    pairs = [(source, (source + steps) % count) for source in range(count)]
    return lax.ppermute(value, axis, pairs)


def from_behind(block, axis, distance):
    devices = range(lax.axis_size(axis))
    route = [(i - distance, i) for i in devices if i - distance in devices]
    return lax.ppermute(block, axis, route)


def padded(block, sides, width, periodic):
    for axis, dim in sides:
        count = lax.axis_size(axis)
        forward = [(i, i + 1) for i in range(count - 1)]
        if periodic:
            forward.append((count - 1, 0))
        backward = [(target, source) for source, target in forward]
        low = lax.ppermute(
            lax.slice_in_dim(block, block.shape[dim] - width, None, axis=dim), axis, forward
        )
        high = lax.ppermute(lax.slice_in_dim(block, 0, width, axis=dim), axis, backward)
        block = jnp.concatenate([low, block, high], axis=dim)
    return block


def with_halo(value, sides, width):
    edges = {}
    for axis, dim in sides:
        peers, length = (lax.axis_size(axis), value.shape[dim])
        up = [(i, (i + 1) % peers) for i in range(peers - 1)]
        last = lax.slice_in_dim(value, length - width, length, axis=dim)
        initial = lax.slice_in_dim(value, 0, width, axis=dim)
        edges[dim] = (
            lax.ppermute(last, axis, up),
            lax.ppermute(initial, axis, [(b, a) for a, b in up]),
        )
    done = []
    for _, dim in sides:
        low, high = edges[dim]
        around = [(width, width) if d in done else (0, 0) for d in range(value.ndim)]
        value = jnp.concatenate([jnp.pad(low, around), value, jnp.pad(high, around)], axis=dim)
        done.append(dim)
    return value


def near_and_far(count, near):
    near_groups = [[first + step for step in range(near)] for first in range(0, count, near)]
    far_groups = [[first + near * step for step in range(count // near)] for first in range(near)]
    return near_groups, far_groups


def radix_of(count):
    near = 1
    while near * near < count:
        near *= 2
    return near if count % near == 0 else count


def exchanged(tiles, axis, groups=None):
    return lax.all_to_all(tiles, axis, 0, 0, tiled=True, axis_index_groups=groups)


def summed(tiles):
    return tiles.astype(jnp.float32).sum(axis=0).astype(jnp.bfloat16)


def spread_to(value, peers, axis, groups=None):
    tiles = exchanged(jnp.broadcast_to(value[None], (peers, *value.shape)), axis, groups)
    return tiles.reshape(peers * value.shape[0], *value.shape[1:])


def sum_over_cells(value):
    lats, halves, lons = lax.axis_size("lat"), lax.axis_size("ch"), lax.axis_size("lon")
    rows, width = value.shape
    near = radix_of(lons)
    far = lons // near
    near_groups, far_groups = near_and_far(lons, near)
    tiles = value.reshape(lats, rows // lats, halves, width // halves)
    tiles = jnp.swapaxes(tiles, 1, 2).reshape(lats * halves, rows // lats, width // halves)
    own = summed(exchanged(tiles, ("lat", "ch")))
    own = summed(exchanged(own.reshape(near, -1, own.shape[-1]), "lon", near_groups))
    own = summed(exchanged(own.reshape(far, -1, own.shape[-1]), "lon", far_groups))
    own = spread_to(own, far, "lon", far_groups)
    own = spread_to(own, near, "lon", near_groups)
    return spread_to(own, lats, "lat").astype(jnp.float32)


def add_edges(middle, to_first, to_last):
    row_count = middle.shape[0]
    rest_pads = [(0, 0)] * (middle.ndim - 1)
    lower = jnp.pad(to_first, [(0, row_count - 1)] + rest_pads)
    upper = jnp.pad(to_last, [(row_count - 1, 0)] + rest_pads)
    return middle + lower + upper


def apply_basis(banded, extended, rows_dev):
    accumulated = None
    for shift_row in range(3):
        term = jnp.einsum(
            "ikjq,iqc->ijkc",
            banded[:, :, shift_row],
            extended[shift_row : shift_row + rows_dev],
            preferred_element_type=jnp.float32,
        )
        accumulated = term if accumulated is None else accumulated + term
    return accumulated


def spread_basis(banded, errors):
    pieces = [
        jnp.einsum(
            "ikjq,ijkc->iqc", banded[:, :, shift_row], errors, preferred_element_type=jnp.float32
        )
        for shift_row in range(3)
    ]
    first = jnp.pad(pieces[0], ((0, 2), (0, 0), (0, 0)))
    second = jnp.pad(pieces[1], ((1, 1), (0, 0), (0, 0)))
    third = jnp.pad(pieces[2], ((2, 0), (0, 0), (0, 0)))
    return first + second + third


def return_rims(spread, cols_dev):
    left_rim = spread[:, :REACH]
    right_rim = spread[:, REACH + cols_dev :]
    interior = spread[:, REACH : REACH + cols_dev]
    from_east = passed_along(left_rim.astype(jnp.bfloat16), "lon", -1).astype(left_rim.dtype)
    from_west = passed_along(right_rim.astype(jnp.bfloat16), "lon", 1).astype(right_rim.dtype)
    interior = interior + jnp.pad(from_west, ((0, 0), (0, cols_dev - REACH), (0, 0)))
    interior = interior + jnp.pad(from_east, ((0, 0), (cols_dev - REACH, 0), (0, 0)))
    row_total = interior.shape[0]
    from_above = from_behind(interior[0:1], ("lat", "ch"), -1)
    from_below = from_behind(interior[row_total - 1 :], ("lat", "ch"), 1)
    return add_edges(interior[1 : row_total - 1], from_below, from_above)


def per_device(
    input_field,
    encoder_filter,
    row_owner,
    encoder_weight,
    disco_basis,
    row_widths,
    block_weights,
    cotangent,
):
    rows_in, cols_in, in_width = input_field.shape
    rows_dev = rows_in // 2
    cols_dev = cols_in // 2
    basis_count = encoder_filter.shape[1]
    tap_count = encoder_filter.shape[2]
    channels = block_weights.shape[2]
    layers = block_weights.shape[0]
    cell_count = rows_dev * cols_dev
    extended_in = padded(input_field, (("lon", 1),), TAP_REACH, True)
    filter_values = encoder_filter.astype(jnp.float32)
    accumulated = jnp.zeros((rows_in, cols_dev, basis_count, in_width), jnp.float32)
    for tap_index in range(tap_count):
        sampled = extended_in[:, tap_index : tap_index + cols_in : 2, :]
        accumulated = (
            accumulated
            + sampled[:, :, None, :].astype(jnp.float32)
            * filter_values[:, None, :, tap_index, None]
        )
    filtered_in = accumulated.astype(jnp.bfloat16).reshape(
        rows_in, cols_dev * basis_count * in_width
    )
    first_row = lax.axis_index(("lat", "ch")) * rows_dev
    relative = row_owner - first_row + 1
    selector = (relative[None, :] == jnp.arange(rows_dev + 2, dtype=jnp.int32)[:, None]).astype(
        jnp.bfloat16
    )
    summed = jnp.dot(selector, filtered_in, preferred_element_type=jnp.float32)
    from_above = from_behind(summed[0:1].astype(jnp.bfloat16), ("lat", "ch"), -1).astype(
        jnp.float32
    )
    from_below = from_behind(summed[rows_dev + 1 :].astype(jnp.bfloat16), ("lat", "ch"), 1).astype(
        jnp.float32
    )
    regridded = add_edges(summed[1 : rows_dev + 1], from_below, from_above)
    latent_in = regridded.astype(jnp.bfloat16).reshape(cell_count, basis_count * in_width)
    current = jnp.dot(latent_in, encoder_weight, preferred_element_type=jnp.float32).astype(
        jnp.bfloat16
    )
    current = current.reshape(rows_dev, cols_dev, channels)
    offsets = jnp.abs(jnp.arange(2 * REACH + 1, dtype=jnp.int32) - REACH)
    keep = offsets[None, :] <= row_widths[:, None]
    masked = jnp.where(keep[:, None, None, :], disco_basis, jnp.zeros_like(disco_basis))
    ext_cols = cols_dev + 2 * REACH
    differences = (
        jnp.arange(ext_cols, dtype=jnp.int32)[None, :]
        - jnp.arange(cols_dev, dtype=jnp.int32)[:, None]
    )
    placement = (
        differences[:, :, None] == jnp.arange(2 * REACH + 1, dtype=jnp.int32)[None, None, :]
    ).astype(jnp.bfloat16)
    banded = jnp.einsum(
        "ikrt,jqt->ikrjq", masked, placement, preferred_element_type=jnp.float32
    ).astype(jnp.bfloat16)
    saved = []
    for layer_index in range(layers):
        rows_ext = with_halo(current, ((("lat", "ch"), 0),), 1)
        extended = padded(rows_ext, (("lon", 1),), REACH, True)
        features = (
            apply_basis(banded, extended, rows_dev)
            .astype(jnp.bfloat16)
            .reshape(cell_count, basis_count * channels)
        )
        preact = jnp.dot(features, block_weights[layer_index], preferred_element_type=jnp.float32)
        current = (
            current.astype(jnp.float32) + jax.nn.silu(preact).reshape(rows_dev, cols_dev, channels)
        ).astype(jnp.bfloat16)
        saved.append((features, preact))
    gradient = cotangent
    weight_terms = [None] * layers
    for layer_index in reversed(range(layers)):
        features, preact = saved[layer_index]
        sigma = jax.nn.sigmoid(preact)
        upstream = gradient.reshape(cell_count, channels).astype(jnp.float32)
        act_grad = (upstream * sigma * (1.0 + preact * (1.0 - sigma))).astype(jnp.bfloat16)
        weight_terms[layer_index] = lax.dot_general(
            features, act_grad, (((0,), (0,)), ((), ())), preferred_element_type=jnp.float32
        )
        errors = lax.dot_general(
            act_grad,
            block_weights[layer_index],
            (((1,), (1,)), ((), ())),
            preferred_element_type=jnp.float32,
        )
        errors = errors.astype(jnp.bfloat16).reshape(rows_dev, cols_dev, basis_count, channels)
        spread = spread_basis(banded, errors)
        returned = return_rims(spread, cols_dev)
        gradient = (gradient.astype(jnp.float32) + returned).astype(jnp.bfloat16)
    encoder_term = lax.dot_general(
        latent_in,
        gradient.reshape(cell_count, channels),
        (((0,), (0,)), ((), ())),
        preferred_element_type=jnp.float32,
    )
    own_width = channels // lax.axis_size("ch")
    grads = jnp.concatenate(weight_terms + [encoder_term], axis=0).astype(jnp.bfloat16)
    grad_sum = sum_over_cells(grads)
    block_rows = layers * basis_count * channels
    block_sum = grad_sum[:block_rows]
    encoder_sum = grad_sum[block_rows:]
    cells_total = cell_count * lax.axis_size("lon") * lax.axis_size(("lat", "ch"))
    normalizer = 1.0 / math.sqrt(cells_total)
    block_grads = (block_sum * normalizer).reshape(layers, basis_count * channels, own_width)
    encoder_grad = encoder_sum * normalizer
    return (current, gradient, block_grads, encoder_grad)


def solution(mesh):
    placed = (
        P(("ens", "lat", "ch"), "lon", None),
        P(("lat", "ch"), None, None),
        P(("ens", "lat", "ch")),
        P(),
        P(("lat", "ch"), None, None, None),
        P(("lat", "ch")),
        P(),
        P(("ens", "lat", "ch"), "lon", None),
    )
    return jax.shard_map(
        per_device,
        mesh=mesh,
        in_specs=placed,
        out_specs=(
            P(("ens", "lat", "ch"), "lon", None),
            P(("ens", "lat", "ch"), "lon", None),
            P("ens", None, "ch"),
            P("ens", "ch"),
        ),
        check_vma=False,
    )
```

```python
import math

import jax
import jax.numpy as jnp
import numpy as np
from jax import lax
from jax.experimental import pallas as pl
from jax.experimental.pallas import tpu as pltpu
from jax.sharding import PartitionSpec as P

REACH = 8
TAP_REACH = 2
LANES = 128
BAND = ("lat", "ch")


def ring_permute(value, axis, steps):
    count = lax.axis_size(axis)
    return lax.ppermute(value, axis, [(i, (i + steps) % count) for i in range(count)])


def line_permute(value, axis, steps):
    count = lax.axis_size(axis)
    pairs = [(i, i + steps) for i in range(count) if 0 <= i + steps < count]
    return lax.ppermute(value, axis, pairs)


def near_and_far(count, near):
    near_groups = [[first + step for step in range(near)] for first in range(0, count, near)]
    far_groups = [[first + near * step for step in range(count // near)] for first in range(near)]
    return near_groups, far_groups


def radix_of(count):
    near = 1
    while near * near < count:
        near *= 2
    return near if count % near == 0 else count


def exchanged(tiles, axis, groups=None):
    return lax.all_to_all(tiles, axis, 0, 0, tiled=True, axis_index_groups=groups)


def summed(tiles):
    return tiles.astype(jnp.float32).sum(axis=0).astype(jnp.bfloat16)


def copies_to(value, peers, axis, groups=None):
    return exchanged(jnp.broadcast_to(value[None], (peers, *value.shape)), axis, groups)


def sum_over_cells(value):
    lats, lons = lax.axis_size("lat"), lax.axis_size("lon")
    rows, width = value.shape
    half = width // lax.axis_size("ch")
    core = lax.axis_index("ch")
    given = lax.dynamic_slice_in_dim(value, (1 - core) * half, half, 1)
    kept = lax.dynamic_slice_in_dim(value, core * half, half, 1)
    taken = ring_permute(given, "ch", 1)
    own = (kept.astype(jnp.float32) + taken.astype(jnp.float32)).astype(jnp.bfloat16)
    near = radix_of(lons)
    far = lons // near
    near_groups, far_groups = near_and_far(lons, near)
    own = summed(exchanged(own.reshape(lats, rows // lats, half), "lat"))
    own = summed(exchanged(own.reshape(near, -1, half), "lon", near_groups))
    own = summed(copies_to(own, far, "lon", far_groups))
    own = copies_to(own, near, "lon", near_groups).reshape(-1, half)
    return copies_to(own, lats, "lat").reshape(rows, half).astype(jnp.float32)


def placement(basis_count, span):
    taps = span - 1
    blocks = []

    def source(k, r, t):
        return (k * 3 + r) * span + t

    for k in range(basis_count):
        wide = np.zeros((basis_count * 3 * span, 2 * LANES), np.float32)
        for r in range(3):
            for t in range(span):
                wide[source(k, r, t), r * 64 + t] = 1
        blocks.append(wide)
    for k in range(basis_count):
        thin = np.zeros((basis_count * 3 * span, LANES), np.float32)
        for r in range(3):
            for t in range(span):
                thin[source(k, r, t), r * 32 + t] = 1
        blocks.append(thin)
    for r in range(3):
        wide = np.zeros((basis_count * 3 * span, 2 * LANES), np.float32)
        for k in range(basis_count):
            for t in range(span):
                wide[source(k, r, t), k * 64 + taps - t] = 1
        blocks.append(wide)
    for r in range(3):
        thin = np.zeros((basis_count * 3 * span, LANES), np.float32)
        for k in range(basis_count):
            for t in range(span):
                thin[source(k, r, t), k * 32 + taps - t] = 1
        blocks.append(thin)
    return np.concatenate(blocks, axis=1)


FORWARD_WIDE, FORWARD_THIN, BACKWARD_WIDE, BACKWARD_THIN = 0, 8, 12, 18


def slanted(vecs, row, block, height):
    vector = vecs[row : row + 1, block * LANES : (block + 1) * LANES]
    spread = jnp.broadcast_to(vector, (height, LANES))
    return pltpu.roll(spread, 0, 1, stride=1, stride_axis=0).astype(jnp.bfloat16)


def dot(left, right):
    return jnp.dot(left, right, preferred_element_type=jnp.float32)


def dot_nt(left, right):
    return lax.dot_general(
        left, right, (((1,), (1,)), ((), ())), preferred_element_type=jnp.float32
    )


def forward_kernel(
    vecs, own, west, east, weights, cot, feat0, pre0, feat1, state2, act1, s0, wide, s1
):
    rows, cols = cot.shape[0], cot.shape[1]
    channels = cot.shape[2]
    basis_count = weights.shape[1] // channels
    mid = cols + 2 * REACH
    for i in range(rows + 4):
        s0[i * 64 : i * 64 + cols] = west[i * cols : (i + 1) * cols]
        s0[i * 64 + cols : i * 64 + 2 * cols] = own[i]
        s0[i * 64 + 2 * cols : i * 64 + 3 * cols] = east[i * cols : (i + 1) * cols]
        s0[i * 64 + 3 * cols : (i + 1) * 64] = jnp.zeros((64 - 3 * cols, channels), jnp.bfloat16)
    s0[(rows + 4) * 64 :] = jnp.zeros((64, channels), jnp.bfloat16)
    for i in range(rows + 2):
        band = jnp.concatenate(
            [
                jnp.concatenate(
                    [slanted(vecs, i + 1, FORWARD_WIDE + 2 * k + h, mid) for h in range(2)],
                    axis=1,
                )
                for k in range(basis_count)
            ],
            axis=0,
        )
        out = dot(band, s0[i * 64 : (i + 4) * 64])
        for k in range(basis_count):
            part = out[k * mid : (k + 1) * mid]
            wide[i * mid : (i + 1) * mid, k * channels : (k + 1) * channels] = part.astype(
                jnp.bfloat16
            )
            if 1 <= i <= rows:
                feat0[(i - 1) * cols : i * cols, k * channels : (k + 1) * channels] = part[
                    REACH : REACH + cols
                ].astype(jnp.bfloat16)
    pre0[...] = dot(wide[...], weights[0])
    for i in range(rows + 2):
        pre = pre0[i * mid : (i + 1) * mid]
        before = s0[(i + 1) * 64 : (i + 1) * 64 + 3 * cols].astype(jnp.float32)
        before = before[REACH : REACH + mid]
        s1[i * mid : (i + 1) * mid] = (before + pre * jax.nn.sigmoid(pre)).astype(jnp.bfloat16)
    s1[(rows + 2) * mid :] = jnp.zeros((mid, channels), jnp.bfloat16)
    for i in range(rows):
        band = jnp.concatenate(
            [slanted(vecs, i + 2, FORWARD_THIN + k, cols) for k in range(basis_count)], axis=0
        )
        out = dot(band, s1[i * mid : (i + 4) * mid])
        for k in range(basis_count):
            feat1[i * cols : (i + 1) * cols, k * channels : (k + 1) * channels] = out[
                k * cols : (k + 1) * cols
            ].astype(jnp.bfloat16)
    pre1 = dot(feat1[...], weights[1])
    for i in range(rows):
        pre = pre1[i * cols : (i + 1) * cols]
        sigma = jax.nn.sigmoid(pre)
        before = s1[(i + 1) * mid : (i + 2) * mid].astype(jnp.float32)[REACH : REACH + cols]
        state2[i] = (before + pre * sigma).astype(jnp.bfloat16)
        upstream = cot[i].astype(jnp.float32)
        act1[i] = (upstream * sigma * (1.0 + pre * (1.0 - sigma))).astype(jnp.bfloat16)


def backward_kernel(
    vecs, own, west, east, weights, pre0, cot, west_cot, east_cot, act0, grad0, a1, e1, g1, a0, e0
):
    rows, cols, channels = grad0.shape
    basis_count = weights.shape[1] // channels
    mid = cols + 2 * REACH
    full = 3 * cols
    skip = (rows + 4) * cols
    for i in range(rows + 4):
        a1[i * full : i * full + cols] = west[i]
        a1[i * full + cols : i * full + 2 * cols] = own[i]
        a1[i * full + 2 * cols : (i + 1) * full] = east[i]
    for k in range(basis_count):
        errors = dot_nt(a1[...], weights[1, k * channels : (k + 1) * channels])
        errors = errors.astype(jnp.bfloat16)
        for i in range(rows + 4):
            first = (i * basis_count + k) * 64
            e1[first : first + full] = errors[i * full : (i + 1) * full]
            e1[first + full : first + 64] = jnp.zeros((64 - full, channels), jnp.bfloat16)
    for i in range(rows + 2):
        band = jnp.concatenate(
            [
                slanted(vecs, i + s, BACKWARD_WIDE + (2 - s) * 2 + h, mid)
                for s in range(3)
                for h in range(2)
            ],
            axis=1,
        )
        spread = dot(band, e1[i * basis_count * 64 : (i + 3) * basis_count * 64])
        upstream = jnp.concatenate(
            [
                west_cot[skip + i * REACH : skip + (i + 1) * REACH].astype(jnp.float32),
                cot[i].astype(jnp.float32),
                east_cot[skip + i * REACH : skip + (i + 1) * REACH].astype(jnp.float32),
            ],
            axis=0,
        )
        grad = (upstream + spread).astype(jnp.bfloat16).astype(jnp.float32)
        g1[i * mid : (i + 1) * mid] = grad
        pre = pre0[i * mid : (i + 1) * mid]
        sigma = jax.nn.sigmoid(pre)
        act = grad * sigma * (1.0 + pre * (1.0 - sigma))
        a0[i * mid : (i + 1) * mid] = act.astype(jnp.bfloat16)
        if 1 <= i <= rows:
            act0[(i - 1) * cols : i * cols] = act[REACH : REACH + cols].astype(jnp.bfloat16)
    for k in range(basis_count):
        errors = dot_nt(a0[...], weights[0, k * channels : (k + 1) * channels])
        errors = errors.astype(jnp.bfloat16)
        for i in range(rows + 2):
            first = (i * basis_count + k) * mid
            e0[first : first + mid] = errors[i * mid : (i + 1) * mid]
    for i in range(rows):
        band = jnp.concatenate(
            [slanted(vecs, i + s + 1, BACKWARD_THIN + 2 - s, cols) for s in range(3)], axis=1
        )
        spread = dot(band, e0[i * basis_count * mid : (i + 3) * basis_count * mid])
        before = g1[(i + 1) * mid + REACH : (i + 1) * mid + REACH + cols]
        grad0[i] = (before + spread).astype(jnp.bfloat16)


def in_vmem(count):
    return [pl.BlockSpec(memory_space=pltpu.VMEM)] * count


def run_forward(vecs, own, west, east, weights, cot):
    rows, cols, channels = cot.shape
    depth = weights.shape[1]
    mid = cols + 2 * REACH
    bf16, f32 = jnp.bfloat16, jnp.float32
    return pl.pallas_call(
        forward_kernel,
        out_shape=(
            jax.ShapeDtypeStruct((rows * cols, depth), bf16),
            jax.ShapeDtypeStruct(((rows + 2) * mid, channels), f32),
            jax.ShapeDtypeStruct((rows * cols, depth), bf16),
            jax.ShapeDtypeStruct((rows, cols, channels), bf16),
            jax.ShapeDtypeStruct((rows, cols, channels), bf16),
        ),
        in_specs=in_vmem(6),
        out_specs=tuple(in_vmem(5)),
        scratch_shapes=[
            pltpu.VMEM(((rows + 5) * 64, channels), bf16),
            pltpu.VMEM(((rows + 2) * mid, depth), bf16),
            pltpu.VMEM(((rows + 3) * mid, channels), bf16),
        ],
        name="forward",
    )(vecs, own, west, east, weights, cot)


def run_backward(vecs, own, west, east, weights, pre0, cot, west_cot, east_cot):
    rows, cols, channels = own.shape
    rows -= 4
    basis_count = weights.shape[1] // channels
    mid = cols + 2 * REACH
    bf16, f32 = jnp.bfloat16, jnp.float32
    return pl.pallas_call(
        backward_kernel,
        out_shape=(
            jax.ShapeDtypeStruct((rows * cols, channels), bf16),
            jax.ShapeDtypeStruct((rows, cols, channels), bf16),
        ),
        in_specs=in_vmem(9),
        out_specs=tuple(in_vmem(2)),
        scratch_shapes=[
            pltpu.VMEM(((rows + 4) * 3 * cols, channels), bf16),
            pltpu.VMEM(((rows + 4) * basis_count * 64, channels), bf16),
            pltpu.VMEM(((rows + 2) * mid, channels), f32),
            pltpu.VMEM(((rows + 2) * mid, channels), bf16),
            pltpu.VMEM(((rows + 2) * basis_count * mid, channels), bf16),
        ],
        name="backward",
    )(vecs, own, west, east, weights, pre0, cot, west_cot, east_cot)


def per_device(
    input_field,
    encoder_filter,
    row_owner,
    encoder_weight,
    disco_basis,
    row_widths,
    block_weights,
    cotangent,
):
    rows_in, cols_in, in_width = input_field.shape
    rows_dev, cols_dev, channels = cotangent.shape
    basis_count, tap_count = encoder_filter.shape[1:]
    layers = block_weights.shape[0]
    span = disco_basis.shape[3]
    cell_count = rows_dev * cols_dev
    latent_width = basis_count * in_width
    f32, bf16 = jnp.float32, jnp.bfloat16

    from_west = ring_permute(input_field[:, cols_in - TAP_REACH :], "lon", 1)
    from_east = ring_permute(input_field[:, :TAP_REACH], "lon", -1)
    offsets = jnp.abs(jnp.arange(span, dtype=jnp.int32) - REACH)
    keep = offsets[None, :] <= row_widths[:, None]
    masked = jnp.where(keep[:, None, None, :], disco_basis, jnp.zeros_like(disco_basis))
    masked = masked.reshape(rows_dev, -1)
    taps_at = (
        np.arange(cols_in + 2 * TAP_REACH)[None, :, None] - 2 * np.arange(cols_dev)[:, None, None]
        == np.arange(tap_count)[None, None, :]
    )
    filters = jnp.einsum(
        "pkt,jqt->pjkq", encoder_filter, jnp.asarray(taps_at, bf16), preferred_element_type=f32
    ).astype(bf16)
    extended_in = jnp.concatenate([from_west, input_field, from_east], axis=1)
    filtered = jnp.einsum("pjkq,pqc->pjkc", filters, extended_in, preferred_element_type=f32)
    filtered = filtered.astype(bf16).reshape(rows_in, cols_dev * latent_width)
    first_row = lax.axis_index(BAND) * rows_dev
    relative = row_owner - first_row + 1
    selector = (relative[None, :] == jnp.arange(rows_dev + 2, dtype=jnp.int32)[:, None]).astype(bf16)
    partial = jnp.dot(selector, filtered, preferred_element_type=f32)
    partial = partial.reshape(rows_dev + 2, cols_dev, latent_width)

    def edge_message(latent_rows, cot_row, basis_rows):
        basis_rows = jnp.pad(basis_rows, ((0, 6), (0, latent_width - basis_rows.shape[1])))
        return jnp.concatenate(
            [
                latent_rows.astype(bf16).reshape(-1, latent_width),
                cot_row.reshape(-1, latent_width),
                basis_rows,
            ]
        )

    above = line_permute(edge_message(partial[-3:], cotangent[-1:], masked[-2:]), BAND, 1)
    below = line_permute(edge_message(partial[:3], cotangent[:1], masked[:2]), BAND, -1)
    lat_rows = 3 * cols_dev
    cot_rows = cols_dev * channels // latent_width

    def opened(message):
        latent = message[:lat_rows].reshape(3, cols_dev, latent_width).astype(f32)
        cot = message[lat_rows : lat_rows + cot_rows].reshape(1, cols_dev, channels)
        return latent, cot, message[lat_rows + cot_rows :][:2, : masked.shape[1]]

    above_latent, above_cot, above_basis = opened(above)
    below_latent, below_cot, below_basis = opened(below)
    tail = rows_dev + 1
    latent = (
        jnp.pad(partial, ((1, 1), (0, 0), (0, 0)))
        + jnp.pad(above_latent, ((0, tail), (0, 0), (0, 0)))
        + jnp.pad(below_latent, ((tail, 0), (0, 0), (0, 0)))
    ).astype(bf16)
    state0 = jnp.dot(
        latent.reshape(-1, latent_width), encoder_weight, preferred_element_type=f32
    ).astype(bf16)
    cot_rows_ext = jnp.concatenate([above_cot, cotangent, below_cot])
    to_east = jnp.concatenate([state0, cot_rows_ext[:, -REACH:].reshape(-1, channels)])
    to_west = jnp.concatenate([state0, cot_rows_ext[:, :REACH].reshape(-1, channels)])
    west = ring_permute(to_east, "lon", 1)
    east = ring_permute(to_west, "lon", -1)
    basis_ext = jnp.concatenate([above_basis, masked, below_basis])
    vecs = jnp.dot(
        basis_ext, jnp.asarray(placement(basis_count, span), bf16), preferred_element_type=f32
    )
    state0 = state0.reshape(rows_dev + 4, cols_dev, channels)
    feat0, pre0, feat1, state_out, act1 = run_forward(
        vecs, state0, west, east, block_weights, cotangent
    )

    act_above = line_permute(act1[-2:], BAND, 1)
    act_below = line_permute(act1[:2], BAND, -1)
    act_rows = jnp.concatenate([act_above, act1, act_below])
    act_west = ring_permute(act_rows, "lon", 1)
    act_east = ring_permute(act_rows, "lon", -1)
    weight1 = lax.dot_general(
        feat1, act1.reshape(cell_count, channels), (((0,), (0,)), ((), ())),
        preferred_element_type=f32,
    )
    act0, gradient = run_backward(
        vecs, act_rows, act_west, act_east, block_weights, pre0, cot_rows_ext, west, east
    )
    weight0 = lax.dot_general(
        feat0, act0, (((0,), (0,)), ((), ())), preferred_element_type=f32
    )
    encoder_term = lax.dot_general(
        latent[2 : rows_dev + 2].reshape(cell_count, latent_width),
        gradient.reshape(cell_count, channels),
        (((0,), (0,)), ((), ())),
        preferred_element_type=f32,
    )
    grads = jnp.concatenate([weight0, weight1, encoder_term], axis=0).astype(bf16)
    grad_sum = sum_over_cells(grads)
    block_rows = layers * basis_count * channels
    cells_total = cell_count * lax.axis_size("lon") * lax.axis_size(BAND)
    normalizer = 1.0 / math.sqrt(cells_total)
    block_grads = (grad_sum[:block_rows] * normalizer).reshape(
        layers, basis_count * channels, grad_sum.shape[1]
    )
    return (state_out, gradient, block_grads, grad_sum[block_rows:] * normalizer)


def solution(mesh):
    placed = (
        P(("ens", "lat", "ch"), "lon", None),
        P(("lat", "ch"), None, None),
        P(("ens", "lat", "ch")),
        P(),
        P(("lat", "ch"), None, None, None),
        P(("lat", "ch")),
        P(),
        P(("ens", "lat", "ch"), "lon", None),
    )
    return jax.shard_map(
        per_device,
        mesh=mesh,
        in_specs=placed,
        out_specs=(
            P(("ens", "lat", "ch"), "lon", None),
            P(("ens", "lat", "ch"), "lon", None),
            P("ens", None, "ch"),
            P("ens", "ch"),
        ),
        check_vma=False,
    )
```

```python
import math

import jax
import jax.numpy as jnp
import numpy as np
from jax import lax
from jax.experimental import pallas as pl
from jax.experimental.pallas import tpu as pltpu
from jax.sharding import PartitionSpec as P

REACH = 8
TAP_REACH = 2
LANES = 128
BAND = ("lat", "ch")


def ring_permute(value, axis, steps):
    count = lax.axis_size(axis)
    return lax.ppermute(value, axis, [(i, (i + steps) % count) for i in range(count)])


def line_permute(value, axis, steps):
    count = lax.axis_size(axis)
    pairs = [(i, i + steps) for i in range(count) if 0 <= i + steps < count]
    return lax.ppermute(value, axis, pairs)


def near_and_far(count, near):
    near_groups = [[first + step for step in range(near)] for first in range(0, count, near)]
    far_groups = [[first + near * step for step in range(count // near)] for first in range(near)]
    return near_groups, far_groups


def radix_of(count):
    near = 1
    while near * near < count:
        near *= 2
    return near if count % near == 0 else count


def exchanged(tiles, axis, groups=None):
    return lax.all_to_all(tiles, axis, 0, 0, tiled=True, axis_index_groups=groups)


def summed(tiles):
    return tiles.astype(jnp.float32).sum(axis=0).astype(jnp.bfloat16)


def copies_to(value, peers, axis, groups=None):
    return exchanged(jnp.broadcast_to(value[None], (peers, *value.shape)), axis, groups)


def sum_over_cells(value):
    lats, lons = lax.axis_size("lat"), lax.axis_size("lon")
    rows, width = value.shape
    half = width // lax.axis_size("ch")
    core = lax.axis_index("ch")
    given = lax.dynamic_slice_in_dim(value, (1 - core) * half, half, 1)
    kept = lax.dynamic_slice_in_dim(value, core * half, half, 1)
    taken = ring_permute(given, "ch", 1)
    own = (kept.astype(jnp.float32) + taken.astype(jnp.float32)).astype(jnp.bfloat16)
    near = radix_of(lons)
    far = lons // near
    near_groups, far_groups = near_and_far(lons, near)
    own = summed(exchanged(own.reshape(lats, rows // lats, half), "lat"))
    own = summed(exchanged(own.reshape(near, -1, half), "lon", near_groups))
    own = summed(copies_to(own, far, "lon", far_groups))
    own = copies_to(own, near, "lon", near_groups).reshape(-1, half)
    return copies_to(own, lats, "lat").reshape(rows, half).astype(jnp.float32)


def placement(basis_count, span):
    taps = span - 1
    blocks = []

    def source(k, r, t):
        return (k * 3 + r) * span + t

    for k in range(basis_count):
        wide = np.zeros((basis_count * 3 * span, 2 * LANES), np.float32)
        for r in range(3):
            for t in range(span):
                wide[source(k, r, t), r * 64 + t] = 1
        blocks.append(wide)
    for k in range(basis_count):
        thin = np.zeros((basis_count * 3 * span, LANES), np.float32)
        for r in range(3):
            for t in range(span):
                thin[source(k, r, t), r * 32 + t] = 1
        blocks.append(thin)
    for r in range(3):
        wide = np.zeros((basis_count * 3 * span, 2 * LANES), np.float32)
        for k in range(basis_count):
            for t in range(span):
                wide[source(k, r, t), k * 64 + taps - t] = 1
        blocks.append(wide)
    for r in range(3):
        thin = np.zeros((basis_count * 3 * span, LANES), np.float32)
        for k in range(basis_count):
            for t in range(span):
                thin[source(k, r, t), k * 32 + taps - t] = 1
        blocks.append(thin)
    return np.concatenate(blocks, axis=1)


FORWARD_WIDE, FORWARD_THIN, BACKWARD_WIDE, BACKWARD_THIN = 0, 8, 12, 18


def slanted(vecs, row, block, height):
    vector = vecs[row : row + 1, block * LANES : (block + 1) * LANES]
    spread = jnp.broadcast_to(vector, (height, LANES))
    return pltpu.roll(spread, 0, 1, stride=1, stride_axis=0).astype(jnp.bfloat16)


def dot(left, right):
    return jnp.dot(left, right, preferred_element_type=jnp.float32)


def dot_nt(left, right):
    return lax.dot_general(
        left, right, (((1,), (1,)), ((), ())), preferred_element_type=jnp.float32
    )


def forward_kernel(
    vecs, own, west, east, weights, cot, feat0, pre0, feat1, state2, act1, s0, wide, s1
):
    rows, cols, channels = state2.shape
    basis_count = weights.shape[1] // channels
    mid = cols + 2 * REACH
    for i in range(rows + 8):
        s0[i * 64 : i * 64 + cols] = west[i]
        s0[i * 64 + cols : i * 64 + 2 * cols] = own[i]
        s0[i * 64 + 2 * cols : i * 64 + 3 * cols] = east[i]
        s0[i * 64 + 3 * cols : (i + 1) * 64] = jnp.zeros((64 - 3 * cols, channels), jnp.bfloat16)
    s0[(rows + 8) * 64 :] = jnp.zeros((64, channels), jnp.bfloat16)
    for i in range(rows + 6):
        band = jnp.concatenate(
            [
                jnp.concatenate(
                    [slanted(vecs, i, FORWARD_WIDE + 2 * k + h, mid) for h in range(2)], axis=1
                )
                for k in range(basis_count)
            ],
            axis=0,
        )
        out = dot(band, s0[i * 64 : (i + 4) * 64])
        for k in range(basis_count):
            part = out[k * mid : (k + 1) * mid]
            wide[i * mid : (i + 1) * mid, k * channels : (k + 1) * channels] = part.astype(
                jnp.bfloat16
            )
            if 3 <= i < rows + 3:
                feat0[(i - 3) * cols : (i - 2) * cols, k * channels : (k + 1) * channels] = part[
                    REACH : REACH + cols
                ].astype(jnp.bfloat16)
    pre0[...] = dot(wide[...], weights[0])
    for i in range(rows + 6):
        pre = pre0[i * mid : (i + 1) * mid]
        before = s0[(i + 1) * 64 : (i + 1) * 64 + 3 * cols].astype(jnp.float32)
        before = before[REACH : REACH + mid]
        s1[i * mid : (i + 1) * mid] = (before + pre * jax.nn.sigmoid(pre)).astype(jnp.bfloat16)
    s1[(rows + 6) * mid :] = jnp.zeros((mid, channels), jnp.bfloat16)
    for i in range(rows + 4):
        band = jnp.concatenate(
            [slanted(vecs, i + 1, FORWARD_THIN + k, cols) for k in range(basis_count)], axis=0
        )
        out = dot(band, s1[i * mid : (i + 4) * mid])
        for k in range(basis_count):
            feat1[i * cols : (i + 1) * cols, k * channels : (k + 1) * channels] = out[
                k * cols : (k + 1) * cols
            ].astype(jnp.bfloat16)
    pre1 = dot(feat1[...], weights[1])
    for i in range(rows + 4):
        pre = pre1[i * cols : (i + 1) * cols]
        sigma = jax.nn.sigmoid(pre)
        if 2 <= i < rows + 2:
            before = s1[(i + 1) * mid : (i + 2) * mid].astype(jnp.float32)[REACH : REACH + cols]
            state2[i - 2] = (before + pre * sigma).astype(jnp.bfloat16)
        upstream = cot[i].astype(jnp.float32)[REACH : REACH + cols]
        act1[i] = (upstream * sigma * (1.0 + pre * (1.0 - sigma))).astype(jnp.bfloat16)


def backward_kernel(vecs, own, west, east, weights, pre0, cot, act0, grad0, a1, e1, g1, a0, e0):
    rows, cols, channels = grad0.shape
    basis_count = weights.shape[1] // channels
    mid = cols + 2 * REACH
    full = 3 * cols
    for i in range(rows + 4):
        a1[i * full : i * full + cols] = west[i]
        a1[i * full + cols : i * full + 2 * cols] = own[i]
        a1[i * full + 2 * cols : (i + 1) * full] = east[i]
    for k in range(basis_count):
        errors = dot_nt(a1[...], weights[1, k * channels : (k + 1) * channels])
        errors = errors.astype(jnp.bfloat16)
        for i in range(rows + 4):
            first = (i * basis_count + k) * 64
            e1[first : first + full] = errors[i * full : (i + 1) * full]
            e1[first + full : first + 64] = jnp.zeros((64 - full, channels), jnp.bfloat16)
    parts = []
    for i in range(-2, rows + 2):
        row = i + 2
        band = jnp.concatenate(
            [
                jnp.concatenate(
                    [slanted(vecs, row + 1, BACKWARD_WIDE + 2 * r + h, mid) for h in range(2)],
                    axis=1,
                )
                for r in range(3)
            ],
            axis=0,
        )
        parts.append(dot(band, e1[row * basis_count * 64 : (row + 1) * basis_count * 64]))
        if i < 0:
            continue
        spread = (
            parts[i][2 * mid :] + parts[i + 1][mid : 2 * mid] + parts[i + 2][:mid]
        )
        grad = (cot[i + 1].astype(jnp.float32) + spread).astype(jnp.bfloat16).astype(jnp.float32)
        g1[i * mid : (i + 1) * mid] = grad
        pre = pre0[(i + 2) * mid : (i + 3) * mid]
        sigma = jax.nn.sigmoid(pre)
        act = grad * sigma * (1.0 + pre * (1.0 - sigma))
        a0[i * mid : (i + 1) * mid] = act.astype(jnp.bfloat16)
        if 1 <= i <= rows:
            act0[(i - 1) * cols : i * cols] = act[REACH : REACH + cols].astype(jnp.bfloat16)
    for k in range(basis_count):
        errors = dot_nt(a0[...], weights[0, k * channels : (k + 1) * channels])
        errors = errors.astype(jnp.bfloat16)
        for i in range(rows + 2):
            first = (i * basis_count + k) * mid
            e0[first : first + mid] = errors[i * mid : (i + 1) * mid]
    parts = []
    for i in range(-2, rows):
        row = i + 2
        band = jnp.concatenate(
            [slanted(vecs, row + 2, BACKWARD_THIN + r, cols) for r in range(3)], axis=0
        )
        parts.append(dot(band, e0[row * basis_count * mid : (row + 1) * basis_count * mid]))
        if i < 0:
            continue
        spread = parts[i][2 * cols :] + parts[i + 1][cols : 2 * cols] + parts[i + 2][:cols]
        before = g1[(i + 1) * mid + REACH : (i + 1) * mid + REACH + cols]
        grad0[i] = (before + spread).astype(jnp.bfloat16)


def encoder_kernel(
    first, owner, taps, field, west, east, cot, masked, partial, down, up, acc
):
    rows_in, cols_in, width = field.shape
    rows, cols, channels = cot.shape
    basis_count = taps.shape[1]
    depth = cols_in + 16
    steps = lax.broadcasted_iota(jnp.int32, (16, width), 0)
    acc[...] = jnp.zeros_like(acc)
    for p in range(rows_in):
        pieces = []
        for k in range(basis_count):
            vector = jnp.broadcast_to(taps[p, k : k + 1], (cols, LANES))
            pieces.append(pltpu.roll(vector, 0, 1, stride=2, stride_axis=0))
        band = jnp.concatenate(pieces, axis=0).astype(jnp.bfloat16)[:, :depth]
        edges = jnp.zeros((16, width), jnp.float32)
        for t in range(TAP_REACH):
            column = slice(t * width, (t + 1) * width)
            edges = jnp.where(steps == t, east[p : p + 1, column].astype(jnp.float32), edges)
            edges = jnp.where(
                steps == 16 - TAP_REACH + t, west[p : p + 1, column].astype(jnp.float32), edges
            )
        out = dot(band, jnp.concatenate([field[p], edges.astype(jnp.bfloat16)], axis=0))
        target = owner[p] - first[0]
        acc[target] += out.astype(jnp.bfloat16).astype(jnp.float32)
    for i in range(rows + 2):
        for k in range(basis_count):
            part = acc[i, k * cols : (k + 1) * cols]
            columns = slice(k * width, (k + 1) * width)
            partial[i, :, columns] = part
            if i < 5:
                up[i * cols : (i + 1) * cols, columns] = part.astype(jnp.bfloat16)
            if i >= rows - 3:
                n = i - rows + 3
                down[n * cols : (n + 1) * cols, columns] = part.astype(jnp.bfloat16)
    mid = cols + 2 * REACH
    for message, where, kept in ((down, rows - 2, rows - 8), (up, 0, 0)):
        for n in range(2):
            at = rows_in + (where + n) * REACH
            wide = jnp.concatenate(
                [
                    west[at : at + REACH].astype(jnp.float32),
                    cot[where + n].astype(jnp.float32),
                    east[at : at + REACH].astype(jnp.float32),
                ],
                axis=0,
            )
            message[5 * cols : 5 * cols + mid, n * channels : (n + 1) * channels] = wide.astype(
                jnp.bfloat16
            )
        message[5 * cols + mid :] = jnp.zeros((8, 2 * channels), jnp.bfloat16)
        message[5 * cols + mid :, : masked.shape[1]] = masked[kept : kept + 8]


def in_vmem(count):
    return [pl.BlockSpec(memory_space=pltpu.VMEM)] * count


GRANT = pltpu.CompilerParams(vmem_limit_bytes=26 * 2**20)


def run_encoder(first, owner, taps, field, west, east, cot, masked):
    rows, cols, channels = cot.shape
    basis_count, width = taps.shape[1], field.shape[2]
    message = jax.ShapeDtypeStruct((5 * cols + cols + 2 * REACH + 8, 2 * channels), jnp.bfloat16)
    return pl.pallas_call(
        encoder_kernel,
        out_shape=(
            jax.ShapeDtypeStruct((rows + 2, cols, basis_count * width), jnp.float32),
            message,
            message,
        ),
        in_specs=[pl.BlockSpec(memory_space=pltpu.SMEM)] * 2 + in_vmem(6),
        out_specs=tuple(in_vmem(3)),
        scratch_shapes=[pltpu.VMEM((rows + 2, basis_count * cols, width), jnp.float32)],
        compiler_params=GRANT,
        name="encoder",
    )(first, owner, taps, field, west, east, cot, masked)


def run_forward(vecs, own, west, east, weights, cot):
    rows, cols, channels = own.shape
    rows -= 8
    depth = weights.shape[1]
    mid = cols + 2 * REACH
    bf16, f32 = jnp.bfloat16, jnp.float32
    return pl.pallas_call(
        forward_kernel,
        out_shape=(
            jax.ShapeDtypeStruct((rows * cols, depth), bf16),
            jax.ShapeDtypeStruct(((rows + 6) * mid, channels), f32),
            jax.ShapeDtypeStruct(((rows + 4) * cols, depth), bf16),
            jax.ShapeDtypeStruct((rows, cols, channels), bf16),
            jax.ShapeDtypeStruct((rows + 4, cols, channels), bf16),
        ),
        in_specs=in_vmem(6),
        out_specs=tuple(in_vmem(5)),
        scratch_shapes=[
            pltpu.VMEM(((rows + 9) * 64, channels), bf16),
            pltpu.VMEM(((rows + 6) * mid, depth), bf16),
            pltpu.VMEM(((rows + 7) * mid, channels), bf16),
        ],
        compiler_params=GRANT,
        name="forward",
    )(vecs, own, west, east, weights, cot)


def run_backward(vecs, own, west, east, weights, pre0, cot):
    rows, cols, channels = own.shape
    rows -= 4
    basis_count = weights.shape[1] // channels
    mid = cols + 2 * REACH
    bf16, f32 = jnp.bfloat16, jnp.float32
    return pl.pallas_call(
        backward_kernel,
        out_shape=(
            jax.ShapeDtypeStruct((rows * cols, channels), bf16),
            jax.ShapeDtypeStruct((rows, cols, channels), bf16),
        ),
        in_specs=in_vmem(7),
        out_specs=tuple(in_vmem(2)),
        scratch_shapes=[
            pltpu.VMEM(((rows + 4) * 3 * cols, channels), bf16),
            pltpu.VMEM(((rows + 4) * basis_count * 64, channels), bf16),
            pltpu.VMEM(((rows + 2) * mid, channels), f32),
            pltpu.VMEM(((rows + 2) * mid, channels), bf16),
            pltpu.VMEM(((rows + 2) * basis_count * mid, channels), bf16),
        ],
        compiler_params=GRANT,
        name="backward",
    )(vecs, own, west, east, weights, pre0, cot)


def per_device(
    input_field,
    encoder_filter,
    row_owner,
    encoder_weight,
    disco_basis,
    row_widths,
    block_weights,
    cotangent,
):
    rows_in, cols_in, in_width = input_field.shape
    rows_dev, cols_dev, channels = cotangent.shape
    basis_count, tap_count = encoder_filter.shape[1:]
    layers = block_weights.shape[0]
    span = disco_basis.shape[3]
    cell_count = rows_dev * cols_dev
    latent_width = basis_count * in_width
    f32, bf16 = jnp.float32, jnp.bfloat16

    def side_message(columns, cot_columns):
        return jnp.concatenate(
            [columns.reshape(rows_in, -1), cot_columns.reshape(-1, channels)]
        )

    west_side = ring_permute(
        side_message(input_field[:, cols_in - TAP_REACH :], cotangent[:, cols_dev - REACH :]),
        "lon",
        1,
    )
    east_side = ring_permute(
        side_message(input_field[:, :TAP_REACH], cotangent[:, :REACH]), "lon", -1
    )
    cot_mid = jnp.concatenate(
        [
            west_side[rows_in:].reshape(rows_dev, REACH, channels),
            cotangent,
            east_side[rows_in:].reshape(rows_dev, REACH, channels),
        ],
        axis=1,
    )
    offsets = jnp.abs(jnp.arange(span, dtype=jnp.int32) - REACH)
    keep = offsets[None, :] <= row_widths[:, None]
    masked = jnp.where(keep[:, None, None, :], disco_basis, jnp.zeros_like(disco_basis))
    masked = masked.reshape(rows_dev, -1)
    first_row = lax.axis_index(BAND) * rows_dev - 1
    tap_lanes = np.zeros((tap_count, LANES), np.float32)
    for t in range(tap_count):
        tap_lanes[t, (t - TAP_REACH) % LANES] = 1
        if t < TAP_REACH:
            tap_lanes[t, cols_in + 16 - TAP_REACH + t] = 1
    taps = jnp.einsum(
        "pkt,tl->pkl", encoder_filter, jnp.asarray(tap_lanes, bf16), preferred_element_type=f32
    )
    partial, down, up = run_encoder(
        first_row.reshape(1), row_owner, taps, input_field, west_side, east_side, cotangent, masked
    )
    above = line_permute(down, BAND, 1)
    below = line_permute(up, BAND, -1)
    lat_rows = 5 * cols_dev

    def opened(message, kept):
        latent = message[:lat_rows].reshape(5, cols_dev, latent_width).astype(f32)
        cot = message[lat_rows:-8]
        cot = jnp.stack([cot[:, :channels], cot[:, channels:]])
        return latent, cot, message[-8:][kept, : masked.shape[1]]

    above_latent, above_cot, above_basis = opened(above, slice(5, 8))
    below_latent, below_cot, below_basis = opened(below, slice(0, 3))
    tail = rows_dev + 3
    latent = (
        jnp.pad(partial, ((3, 3), (0, 0), (0, 0)))
        + jnp.pad(above_latent, ((0, tail), (0, 0), (0, 0)))
        + jnp.pad(below_latent, ((tail, 0), (0, 0), (0, 0)))
    ).astype(bf16)
    state0 = jnp.dot(
        latent.reshape(-1, latent_width), encoder_weight, preferred_element_type=f32
    ).astype(bf16)
    state0 = state0.reshape(rows_dev + 8, cols_dev, channels)
    west = ring_permute(state0, "lon", 1)
    east = ring_permute(state0, "lon", -1)
    cot_ext = jnp.concatenate([above_cot, cot_mid, below_cot])
    basis_ext = jnp.concatenate([above_basis, masked, below_basis])
    vecs = jnp.dot(
        basis_ext, jnp.asarray(placement(basis_count, span), bf16), preferred_element_type=f32
    )
    feat0, pre0, feat1, state_out, act1 = run_forward(
        vecs, state0, west, east, block_weights, cot_ext
    )

    act_west = ring_permute(act1, "lon", 1)
    act_east = ring_permute(act1, "lon", -1)
    inner = slice(2 * cols_dev, 2 * cols_dev + cell_count)
    weight1 = lax.dot_general(
        feat1[inner],
        act1.reshape(-1, channels)[inner],
        (((0,), (0,)), ((), ())),
        preferred_element_type=f32,
    )
    act0, gradient = run_backward(
        vecs, act1, act_west, act_east, block_weights, pre0, cot_ext
    )
    weight0 = lax.dot_general(
        feat0, act0, (((0,), (0,)), ((), ())), preferred_element_type=f32
    )
    encoder_term = lax.dot_general(
        latent[4 : rows_dev + 4].reshape(cell_count, latent_width),
        gradient.reshape(cell_count, channels),
        (((0,), (0,)), ((), ())),
        preferred_element_type=f32,
    )
    grads = jnp.concatenate([weight0, weight1, encoder_term], axis=0).astype(bf16)
    grad_sum = sum_over_cells(grads)
    block_rows = layers * basis_count * channels
    cells_total = cell_count * lax.axis_size("lon") * lax.axis_size(BAND)
    normalizer = 1.0 / math.sqrt(cells_total)
    block_grads = (grad_sum[:block_rows] * normalizer).reshape(
        layers, basis_count * channels, grad_sum.shape[1]
    )
    return (state_out, gradient, block_grads, grad_sum[block_rows:] * normalizer)


def solution(mesh):
    placed = (
        P(("ens", "lat", "ch"), "lon", None),
        P(("lat", "ch"), None, None),
        P(("ens", "lat", "ch")),
        P(),
        P(("lat", "ch"), None, None, None),
        P(("lat", "ch")),
        P(),
        P(("ens", "lat", "ch"), "lon", None),
    )
    return jax.shard_map(
        per_device,
        mesh=mesh,
        in_specs=placed,
        out_specs=(
            P(("ens", "lat", "ch"), "lon", None),
            P(("ens", "lat", "ch"), "lon", None),
            P("ens", None, "ch"),
            P("ens", "ch"),
        ),
        check_vma=False,
    )
```

```python
import math

import jax
import jax.numpy as jnp
import numpy as np
from jax import lax
from jax.experimental import pallas as pl
from jax.experimental.pallas import tpu as pltpu
from jax.sharding import PartitionSpec as P

REACH = 8
TAP_REACH = 2
LANES = 128
BAND = ("lat", "ch")


def ring_permute(value, axis, steps):
    count = lax.axis_size(axis)
    return lax.ppermute(value, axis, [(i, (i + steps) % count) for i in range(count)])


def line_permute(value, axis, steps):
    count = lax.axis_size(axis)
    pairs = [(i, i + steps) for i in range(count) if 0 <= i + steps < count]
    return lax.ppermute(value, axis, pairs)


def ring_groups(count, near):
    places = [(place - near // 2) % count for place in range(count)]
    runs = [places[first : first + near] for first in range(0, count, near)]
    return runs


def radix_of(count):
    near = 1
    while near * near < count:
        near *= 2
    return near if count % near == 0 else count


def exchanged(tiles, axis, groups=None):
    return lax.all_to_all(tiles, axis, 0, 0, tiled=True, axis_index_groups=groups)


def summed(tiles):
    return tiles.astype(jnp.float32).sum(axis=0).astype(jnp.bfloat16)


def copies_to(value, peers, axis, groups=None):
    return exchanged(jnp.broadcast_to(value[None], (peers, *value.shape)), axis, groups)


def sum_of_runs(value, axis, runs):
    if len(runs) != 4:
        peers = [list(group) for group in zip(*runs)]
        return summed(copies_to(value, len(runs), axis, peers))
    near = len(runs[0])
    count = len(runs) * near
    run = ((lax.axis_index(axis) + near // 2) % count) // near

    def sent(block, moves):
        pairs = [pair for source, target in moves for pair in zip(runs[source], runs[target])]
        return lax.ppermute(block, axis, pairs).astype(jnp.float32)

    own = value.astype(jnp.float32)
    middle = (run == 1) | (run == 2)
    by_middle = sent(value, [(1, 2), (2, 1)])
    pair = own + by_middle
    by_side = sent(jnp.where(middle, pair, own), [(0, 1), (1, 0), (2, 3), (3, 2)])
    by_seam = sent(value, [(0, 3), (3, 0)])
    by_far = sent(value, [(0, 2), (3, 1)])
    one_and_two = jnp.where(middle, pair, by_side)
    three = jnp.where(
        run == 3, own, jnp.where(run == 0, by_seam, jnp.where(run == 1, by_far, by_side))
    )
    zero = jnp.where(
        run == 0, own, jnp.where(run == 1, by_side, jnp.where(run == 2, by_far, by_seam))
    )
    return (one_and_two + three + zero).astype(jnp.bfloat16)


def sum_over_cells(value):
    lats, lons = lax.axis_size("lat"), lax.axis_size("lon")
    rows, width = value.shape
    half = width // lax.axis_size("ch")
    core = lax.axis_index("ch")
    given = lax.dynamic_slice_in_dim(value, (1 - core) * half, half, 1)
    kept = lax.dynamic_slice_in_dim(value, core * half, half, 1)
    taken = ring_permute(given, "ch", 1)
    own = (kept.astype(jnp.float32) + taken.astype(jnp.float32)).astype(jnp.bfloat16)
    near = radix_of(lons)
    runs = ring_groups(lons, near)
    own = summed(exchanged(own.reshape(lats, rows // lats, half), "lat"))
    own = summed(exchanged(own.reshape(near, -1, half), "lon", runs))
    own = sum_of_runs(own, "lon", runs)
    own = copies_to(own, near, "lon", runs).reshape(-1, half)
    return copies_to(own, lats, "lat").reshape(rows, half).astype(jnp.float32)


def placement(basis_count, span):
    taps = span - 1
    blocks = []

    def source(k, r, t):
        return (k * 3 + r) * span + t

    for k in range(basis_count):
        wide = np.zeros((basis_count * 3 * span, 2 * LANES), np.float32)
        for r in range(3):
            for t in range(span):
                wide[source(k, r, t), r * 64 + t] = 1
        blocks.append(wide)
    for k in range(basis_count):
        thin = np.zeros((basis_count * 3 * span, LANES), np.float32)
        for r in range(3):
            for t in range(span):
                thin[source(k, r, t), r * 32 + t] = 1
        blocks.append(thin)
    for r in range(3):
        wide = np.zeros((basis_count * 3 * span, 2 * LANES), np.float32)
        for k in range(basis_count):
            for t in range(span):
                wide[source(k, r, t), k * 64 + taps - t] = 1
        blocks.append(wide)
    for r in range(3):
        thin = np.zeros((basis_count * 3 * span, LANES), np.float32)
        for k in range(basis_count):
            for t in range(span):
                thin[source(k, r, t), k * 32 + taps - t] = 1
        blocks.append(thin)
    return np.concatenate(blocks, axis=1)


FORWARD_WIDE, FORWARD_THIN, BACKWARD_WIDE, BACKWARD_THIN = 0, 8, 12, 18


def slanted(vecs, row, block, height):
    vector = vecs[row : row + 1, block * LANES : (block + 1) * LANES]
    spread = jnp.broadcast_to(vector, (height, LANES))
    return pltpu.roll(spread, 0, 1, stride=1, stride_axis=0).astype(jnp.bfloat16)


def dot(left, right):
    return jnp.dot(left, right, preferred_element_type=jnp.float32)


def dot_nt(left, right):
    return lax.dot_general(
        left, right, (((1,), (1,)), ((), ())), preferred_element_type=jnp.float32
    )


def forward_kernel(
    vecs, own, west, east, weights, cot, feat0, pre0, feat1, state2, act1, s0, wide, s1
):
    rows, cols, channels = state2.shape
    basis_count = weights.shape[1] // channels
    mid = cols + 2 * REACH
    for i in range(rows + 8):
        s0[i * 64 : i * 64 + cols] = west[i]
        s0[i * 64 + cols : i * 64 + 2 * cols] = own[i]
        s0[i * 64 + 2 * cols : i * 64 + 3 * cols] = east[i]
        s0[i * 64 + 3 * cols : (i + 1) * 64] = jnp.zeros((64 - 3 * cols, channels), jnp.bfloat16)
    s0[(rows + 8) * 64 :] = jnp.zeros((64, channels), jnp.bfloat16)
    for i in range(rows + 6):
        band = jnp.concatenate(
            [
                jnp.concatenate(
                    [slanted(vecs, i, FORWARD_WIDE + 2 * k + h, mid) for h in range(2)], axis=1
                )
                for k in range(basis_count)
            ],
            axis=0,
        )
        out = dot(band, s0[i * 64 : (i + 4) * 64])
        for k in range(basis_count):
            part = out[k * mid : (k + 1) * mid]
            wide[i * mid : (i + 1) * mid, k * channels : (k + 1) * channels] = part.astype(
                jnp.bfloat16
            )
            if 3 <= i < rows + 3:
                feat0[(i - 3) * cols : (i - 2) * cols, k * channels : (k + 1) * channels] = part[
                    REACH : REACH + cols
                ].astype(jnp.bfloat16)
    pre0[...] = dot(wide[...], weights[0])
    for i in range(rows + 6):
        pre = pre0[i * mid : (i + 1) * mid]
        before = s0[(i + 1) * 64 : (i + 1) * 64 + 3 * cols].astype(jnp.float32)
        before = before[REACH : REACH + mid]
        s1[i * mid : (i + 1) * mid] = (before + pre * jax.nn.sigmoid(pre)).astype(jnp.bfloat16)
    s1[(rows + 6) * mid :] = jnp.zeros((mid, channels), jnp.bfloat16)
    for i in range(rows + 4):
        band = jnp.concatenate(
            [slanted(vecs, i + 1, FORWARD_THIN + k, cols) for k in range(basis_count)], axis=0
        )
        out = dot(band, s1[i * mid : (i + 4) * mid])
        for k in range(basis_count):
            feat1[i * cols : (i + 1) * cols, k * channels : (k + 1) * channels] = out[
                k * cols : (k + 1) * cols
            ].astype(jnp.bfloat16)
    pre1 = dot(feat1[...], weights[1])
    for i in range(rows + 4):
        pre = pre1[i * cols : (i + 1) * cols]
        sigma = jax.nn.sigmoid(pre)
        if 2 <= i < rows + 2:
            before = s1[(i + 1) * mid : (i + 2) * mid].astype(jnp.float32)[REACH : REACH + cols]
            state2[i - 2] = (before + pre * sigma).astype(jnp.bfloat16)
        upstream = cot[i].astype(jnp.float32)[REACH : REACH + cols]
        act1[i] = (upstream * sigma * (1.0 + pre * (1.0 - sigma))).astype(jnp.bfloat16)


def backward_kernel(vecs, own, west, east, weights, pre0, cot, act0, grad0, a1, e1, g1, a0, e0):
    rows, cols, channels = grad0.shape
    basis_count = weights.shape[1] // channels
    mid = cols + 2 * REACH
    full = 3 * cols
    for i in range(rows + 4):
        a1[i * full : i * full + cols] = west[i]
        a1[i * full + cols : i * full + 2 * cols] = own[i]
        a1[i * full + 2 * cols : (i + 1) * full] = east[i]
    for k in range(basis_count):
        errors = dot_nt(a1[...], weights[1, k * channels : (k + 1) * channels])
        errors = errors.astype(jnp.bfloat16)
        for i in range(rows + 4):
            first = (i * basis_count + k) * 64
            e1[first : first + full] = errors[i * full : (i + 1) * full]
            e1[first + full : first + 64] = jnp.zeros((64 - full, channels), jnp.bfloat16)
    parts = []
    for i in range(-2, rows + 2):
        row = i + 2
        band = jnp.concatenate(
            [
                jnp.concatenate(
                    [slanted(vecs, row + 1, BACKWARD_WIDE + 2 * r + h, mid) for h in range(2)],
                    axis=1,
                )
                for r in range(3)
            ],
            axis=0,
        )
        parts.append(dot(band, e1[row * basis_count * 64 : (row + 1) * basis_count * 64]))
        if i < 0:
            continue
        spread = (
            parts[i][2 * mid :] + parts[i + 1][mid : 2 * mid] + parts[i + 2][:mid]
        )
        grad = (cot[i + 1].astype(jnp.float32) + spread).astype(jnp.bfloat16).astype(jnp.float32)
        g1[i * mid : (i + 1) * mid] = grad
        pre = pre0[(i + 2) * mid : (i + 3) * mid]
        sigma = jax.nn.sigmoid(pre)
        act = grad * sigma * (1.0 + pre * (1.0 - sigma))
        a0[i * mid : (i + 1) * mid] = act.astype(jnp.bfloat16)
        if 1 <= i <= rows:
            act0[(i - 1) * cols : i * cols] = act[REACH : REACH + cols].astype(jnp.bfloat16)
    for k in range(basis_count):
        errors = dot_nt(a0[...], weights[0, k * channels : (k + 1) * channels])
        errors = errors.astype(jnp.bfloat16)
        for i in range(rows + 2):
            first = (i * basis_count + k) * mid
            e0[first : first + mid] = errors[i * mid : (i + 1) * mid]
    parts = []
    for i in range(-2, rows):
        row = i + 2
        band = jnp.concatenate(
            [slanted(vecs, row + 2, BACKWARD_THIN + r, cols) for r in range(3)], axis=0
        )
        parts.append(dot(band, e0[row * basis_count * mid : (row + 1) * basis_count * mid]))
        if i < 0:
            continue
        spread = parts[i][2 * cols :] + parts[i + 1][cols : 2 * cols] + parts[i + 2][:cols]
        before = g1[(i + 1) * mid + REACH : (i + 1) * mid + REACH + cols]
        grad0[i] = (before + spread).astype(jnp.bfloat16)


def encoder_kernel(
    first, owner, taps, field, west, east, cot, masked, partial, down, up, acc
):
    rows_in, cols_in, width = field.shape
    rows, cols, channels = cot.shape
    basis_count = taps.shape[1]
    depth = cols_in + 16
    steps = lax.broadcasted_iota(jnp.int32, (16, width), 0)
    acc[...] = jnp.zeros_like(acc)
    for p in range(rows_in):
        pieces = []
        for k in range(basis_count):
            vector = jnp.broadcast_to(taps[p, k : k + 1], (cols, LANES))
            pieces.append(pltpu.roll(vector, 0, 1, stride=2, stride_axis=0))
        band = jnp.concatenate(pieces, axis=0).astype(jnp.bfloat16)[:, :depth]
        edges = jnp.zeros((16, width), jnp.float32)
        for t in range(TAP_REACH):
            column = slice(t * width, (t + 1) * width)
            edges = jnp.where(steps == t, east[p : p + 1, column].astype(jnp.float32), edges)
            edges = jnp.where(
                steps == 16 - TAP_REACH + t, west[p : p + 1, column].astype(jnp.float32), edges
            )
        out = dot(band, jnp.concatenate([field[p], edges.astype(jnp.bfloat16)], axis=0))
        target = owner[p] - first[0]
        acc[target] += out.astype(jnp.bfloat16).astype(jnp.float32)
    for i in range(rows + 2):
        for k in range(basis_count):
            part = acc[i, k * cols : (k + 1) * cols]
            columns = slice(k * width, (k + 1) * width)
            partial[i, :, columns] = part
            if i < 5:
                up[i * cols : (i + 1) * cols, columns] = part.astype(jnp.bfloat16)
            if i >= rows - 3:
                n = i - rows + 3
                down[n * cols : (n + 1) * cols, columns] = part.astype(jnp.bfloat16)
    mid = cols + 2 * REACH
    for message, where, kept in ((down, rows - 2, rows - 8), (up, 0, 0)):
        for n in range(2):
            at = rows_in + (where + n) * REACH
            wide = jnp.concatenate(
                [
                    west[at : at + REACH].astype(jnp.float32),
                    cot[where + n].astype(jnp.float32),
                    east[at : at + REACH].astype(jnp.float32),
                ],
                axis=0,
            )
            message[5 * cols : 5 * cols + mid, n * channels : (n + 1) * channels] = wide.astype(
                jnp.bfloat16
            )
        message[5 * cols + mid :] = jnp.zeros((8, 2 * channels), jnp.bfloat16)
        message[5 * cols + mid :, : masked.shape[1]] = masked[kept : kept + 8]


def in_vmem(count):
    return [pl.BlockSpec(memory_space=pltpu.VMEM)] * count


GRANT = pltpu.CompilerParams(vmem_limit_bytes=26 * 2**20)


def run_encoder(first, owner, taps, field, west, east, cot, masked):
    rows, cols, channels = cot.shape
    basis_count, width = taps.shape[1], field.shape[2]
    message = jax.ShapeDtypeStruct((5 * cols + cols + 2 * REACH + 8, 2 * channels), jnp.bfloat16)
    return pl.pallas_call(
        encoder_kernel,
        out_shape=(
            jax.ShapeDtypeStruct((rows + 2, cols, basis_count * width), jnp.float32),
            message,
            message,
        ),
        in_specs=[pl.BlockSpec(memory_space=pltpu.SMEM)] * 2 + in_vmem(6),
        out_specs=tuple(in_vmem(3)),
        scratch_shapes=[pltpu.VMEM((rows + 2, basis_count * cols, width), jnp.float32)],
        compiler_params=GRANT,
        name="encoder",
    )(first, owner, taps, field, west, east, cot, masked)


def run_forward(vecs, own, west, east, weights, cot):
    rows, cols, channels = own.shape
    rows -= 8
    depth = weights.shape[1]
    mid = cols + 2 * REACH
    bf16, f32 = jnp.bfloat16, jnp.float32
    return pl.pallas_call(
        forward_kernel,
        out_shape=(
            jax.ShapeDtypeStruct((rows * cols, depth), bf16),
            jax.ShapeDtypeStruct(((rows + 6) * mid, channels), f32),
            jax.ShapeDtypeStruct(((rows + 4) * cols, depth), bf16),
            jax.ShapeDtypeStruct((rows, cols, channels), bf16),
            jax.ShapeDtypeStruct((rows + 4, cols, channels), bf16),
        ),
        in_specs=in_vmem(6),
        out_specs=tuple(in_vmem(5)),
        scratch_shapes=[
            pltpu.VMEM(((rows + 9) * 64, channels), bf16),
            pltpu.VMEM(((rows + 6) * mid, depth), bf16),
            pltpu.VMEM(((rows + 7) * mid, channels), bf16),
        ],
        compiler_params=GRANT,
        name="forward",
    )(vecs, own, west, east, weights, cot)


def run_backward(vecs, own, west, east, weights, pre0, cot):
    rows, cols, channels = own.shape
    rows -= 4
    basis_count = weights.shape[1] // channels
    mid = cols + 2 * REACH
    bf16, f32 = jnp.bfloat16, jnp.float32
    return pl.pallas_call(
        backward_kernel,
        out_shape=(
            jax.ShapeDtypeStruct((rows * cols, channels), bf16),
            jax.ShapeDtypeStruct((rows, cols, channels), bf16),
        ),
        in_specs=in_vmem(7),
        out_specs=tuple(in_vmem(2)),
        scratch_shapes=[
            pltpu.VMEM(((rows + 4) * 3 * cols, channels), bf16),
            pltpu.VMEM(((rows + 4) * basis_count * 64, channels), bf16),
            pltpu.VMEM(((rows + 2) * mid, channels), f32),
            pltpu.VMEM(((rows + 2) * mid, channels), bf16),
            pltpu.VMEM(((rows + 2) * basis_count * mid, channels), bf16),
        ],
        compiler_params=GRANT,
        name="backward",
    )(vecs, own, west, east, weights, pre0, cot)


def per_device(
    input_field,
    encoder_filter,
    row_owner,
    encoder_weight,
    disco_basis,
    row_widths,
    block_weights,
    cotangent,
):
    rows_in, cols_in, in_width = input_field.shape
    rows_dev, cols_dev, channels = cotangent.shape
    basis_count, tap_count = encoder_filter.shape[1:]
    layers = block_weights.shape[0]
    span = disco_basis.shape[3]
    cell_count = rows_dev * cols_dev
    latent_width = basis_count * in_width
    f32, bf16 = jnp.float32, jnp.bfloat16

    def side_message(columns, cot_columns):
        return jnp.concatenate(
            [columns.reshape(rows_in, -1), cot_columns.reshape(-1, channels)]
        )

    west_side = ring_permute(
        side_message(input_field[:, cols_in - TAP_REACH :], cotangent[:, cols_dev - REACH :]),
        "lon",
        1,
    )
    east_side = ring_permute(
        side_message(input_field[:, :TAP_REACH], cotangent[:, :REACH]), "lon", -1
    )
    cot_mid = jnp.concatenate(
        [
            west_side[rows_in:].reshape(rows_dev, REACH, channels),
            cotangent,
            east_side[rows_in:].reshape(rows_dev, REACH, channels),
        ],
        axis=1,
    )
    offsets = jnp.abs(jnp.arange(span, dtype=jnp.int32) - REACH)
    keep = offsets[None, :] <= row_widths[:, None]
    masked = jnp.where(keep[:, None, None, :], disco_basis, jnp.zeros_like(disco_basis))
    masked = masked.reshape(rows_dev, -1)
    first_row = lax.axis_index(BAND) * rows_dev - 1
    tap_lanes = np.zeros((tap_count, LANES), np.float32)
    for t in range(tap_count):
        tap_lanes[t, (t - TAP_REACH) % LANES] = 1
        if t < TAP_REACH:
            tap_lanes[t, cols_in + 16 - TAP_REACH + t] = 1
    taps = jnp.einsum(
        "pkt,tl->pkl", encoder_filter, jnp.asarray(tap_lanes, bf16), preferred_element_type=f32
    )
    partial, down, up = run_encoder(
        first_row.reshape(1), row_owner, taps, input_field, west_side, east_side, cotangent, masked
    )
    above = line_permute(down, BAND, 1)
    below = line_permute(up, BAND, -1)
    lat_rows = 5 * cols_dev

    def opened(message, kept):
        latent = message[:lat_rows].reshape(5, cols_dev, latent_width).astype(f32)
        cot = message[lat_rows:-8]
        cot = jnp.stack([cot[:, :channels], cot[:, channels:]])
        return latent, cot, message[-8:][kept, : masked.shape[1]]

    above_latent, above_cot, above_basis = opened(above, slice(5, 8))
    below_latent, below_cot, below_basis = opened(below, slice(0, 3))
    tail = rows_dev + 3
    latent = (
        jnp.pad(partial, ((3, 3), (0, 0), (0, 0)))
        + jnp.pad(above_latent, ((0, tail), (0, 0), (0, 0)))
        + jnp.pad(below_latent, ((tail, 0), (0, 0), (0, 0)))
    ).astype(bf16)
    state0 = jnp.dot(
        latent.reshape(-1, latent_width), encoder_weight, preferred_element_type=f32
    ).astype(bf16)
    state0 = state0.reshape(rows_dev + 8, cols_dev, channels)
    west = ring_permute(state0, "lon", 1)
    east = ring_permute(state0, "lon", -1)
    cot_ext = jnp.concatenate([above_cot, cot_mid, below_cot])
    basis_ext = jnp.concatenate([above_basis, masked, below_basis])
    vecs = jnp.dot(
        basis_ext, jnp.asarray(placement(basis_count, span), bf16), preferred_element_type=f32
    )
    feat0, pre0, feat1, state_out, act1 = run_forward(
        vecs, state0, west, east, block_weights, cot_ext
    )

    act_west = ring_permute(act1, "lon", 1)
    act_east = ring_permute(act1, "lon", -1)
    inner = slice(2 * cols_dev, 2 * cols_dev + cell_count)
    weight1 = lax.dot_general(
        feat1[inner],
        act1.reshape(-1, channels)[inner],
        (((0,), (0,)), ((), ())),
        preferred_element_type=f32,
    )
    act0, gradient = run_backward(
        vecs, act1, act_west, act_east, block_weights, pre0, cot_ext
    )
    weight0 = lax.dot_general(
        feat0, act0, (((0,), (0,)), ((), ())), preferred_element_type=f32
    )
    encoder_term = lax.dot_general(
        latent[4 : rows_dev + 4].reshape(cell_count, latent_width),
        gradient.reshape(cell_count, channels),
        (((0,), (0,)), ((), ())),
        preferred_element_type=f32,
    )
    grads = jnp.concatenate([weight0, weight1, encoder_term], axis=0).astype(bf16)
    grad_sum = sum_over_cells(grads)
    block_rows = layers * basis_count * channels
    cells_total = cell_count * lax.axis_size("lon") * lax.axis_size(BAND)
    normalizer = 1.0 / math.sqrt(cells_total)
    block_grads = (grad_sum[:block_rows] * normalizer).reshape(
        layers, basis_count * channels, grad_sum.shape[1]
    )
    return (state_out, gradient, block_grads, grad_sum[block_rows:] * normalizer)


def solution(mesh):
    placed = (
        P(("ens", "lat", "ch"), "lon", None),
        P(("lat", "ch"), None, None),
        P(("ens", "lat", "ch")),
        P(),
        P(("lat", "ch"), None, None, None),
        P(("lat", "ch")),
        P(),
        P(("ens", "lat", "ch"), "lon", None),
    )
    return jax.shard_map(
        per_device,
        mesh=mesh,
        in_specs=placed,
        out_specs=(
            P(("ens", "lat", "ch"), "lon", None),
            P(("ens", "lat", "ch"), "lon", None),
            P("ens", None, "ch"),
            P("ens", "ch"),
        ),
        check_vma=False,
    )
```

```python
import math

import jax
import jax.numpy as jnp
import numpy as np
from jax import lax
from jax.experimental import pallas as pl
from jax.experimental.pallas import tpu as pltpu
from jax.sharding import PartitionSpec as P

REACH = 8
TAP_REACH = 2
LANES = 128
BAND = ("lat", "ch")


def ring_permute(value, axis, steps):
    count = lax.axis_size(axis)
    return lax.ppermute(value, axis, [(i, (i + steps) % count) for i in range(count)])


def line_permute(value, axis, steps):
    count = lax.axis_size(axis)
    pairs = [(i, i + steps) for i in range(count) if 0 <= i + steps < count]
    return lax.ppermute(value, axis, pairs)


def ring_groups(count, near):
    places = [(place - near // 2) % count for place in range(count)]
    runs = [places[first : first + near] for first in range(0, count, near)]
    return runs


def radix_of(count):
    near = 1
    while near * near < count:
        near *= 2
    return near if count % near == 0 else count


def exchanged(tiles, axis, groups=None):
    return lax.all_to_all(tiles, axis, 0, 0, tiled=True, axis_index_groups=groups)


def summed(tiles):
    return tiles.astype(jnp.float32).sum(axis=0).astype(jnp.bfloat16)


def copies_to(value, peers, axis, groups=None):
    return exchanged(jnp.broadcast_to(value[None], (peers, *value.shape)), axis, groups)


def sum_over_cells(value):
    lats, lons = lax.axis_size("lat"), lax.axis_size("lon")
    rows, width = value.shape
    half = width // lax.axis_size("ch")
    core = lax.axis_index("ch")
    given = lax.dynamic_slice_in_dim(value, (1 - core) * half, half, 1)
    kept = lax.dynamic_slice_in_dim(value, core * half, half, 1)
    taken = ring_permute(given, "ch", 1)
    own = (kept.astype(jnp.float32) + taken.astype(jnp.float32)).astype(jnp.bfloat16)
    near = radix_of(lons)
    runs = ring_groups(lons, near)
    own = summed(exchanged(own.reshape(lats, rows // lats, half), "lat"))
    own = summed(exchanged(own.reshape(near, -1, half), "lon", runs))
    own = summed(copies_to(own, len(runs), "lon", [list(peers) for peers in zip(*runs)]))
    own = copies_to(own, near, "lon", runs).reshape(-1, half)
    return copies_to(own, lats, "lat").reshape(rows, half).astype(jnp.float32)


def placement(basis_count, span):
    taps = span - 1
    blocks = []

    def source(k, r, t):
        return (k * 3 + r) * span + t

    for k in range(basis_count):
        wide = np.zeros((basis_count * 3 * span, 2 * LANES), np.float32)
        for r in range(3):
            for t in range(span):
                wide[source(k, r, t), r * 64 + t] = 1
        blocks.append(wide)
    for k in range(basis_count):
        thin = np.zeros((basis_count * 3 * span, LANES), np.float32)
        for r in range(3):
            for t in range(span):
                thin[source(k, r, t), r * 32 + t] = 1
        blocks.append(thin)
    for r in range(3):
        wide = np.zeros((basis_count * 3 * span, 2 * LANES), np.float32)
        for k in range(basis_count):
            for t in range(span):
                wide[source(k, r, t), k * 64 + taps - t] = 1
        blocks.append(wide)
    for r in range(3):
        thin = np.zeros((basis_count * 3 * span, LANES), np.float32)
        for k in range(basis_count):
            for t in range(span):
                thin[source(k, r, t), k * 32 + taps - t] = 1
        blocks.append(thin)
    return np.concatenate(blocks, axis=1)


FORWARD_WIDE, FORWARD_THIN, BACKWARD_WIDE, BACKWARD_THIN = 0, 8, 12, 18


def slanted(vecs, row, block, height):
    vector = vecs[row : row + 1, block * LANES : (block + 1) * LANES]
    spread = jnp.broadcast_to(vector, (height, LANES))
    return pltpu.roll(spread, 0, 1, stride=1, stride_axis=0).astype(jnp.bfloat16)


def dot(left, right):
    return jnp.dot(left, right, preferred_element_type=jnp.float32)


def dot_nt(left, right):
    return lax.dot_general(
        left, right, (((1,), (1,)), ((), ())), preferred_element_type=jnp.float32
    )


def forward_kernel(
    vecs, own, west, east, weights, cot, feat0, pre0, feat1, state2, act1, s0, wide, s1
):
    rows, cols, channels = state2.shape
    basis_count = weights.shape[1] // channels
    mid = cols + 2 * REACH
    for i in range(rows + 8):
        s0[i * 64 : i * 64 + cols] = west[i]
        s0[i * 64 + cols : i * 64 + 2 * cols] = own[i]
        s0[i * 64 + 2 * cols : i * 64 + 3 * cols] = east[i]
        s0[i * 64 + 3 * cols : (i + 1) * 64] = jnp.zeros((64 - 3 * cols, channels), jnp.bfloat16)
    s0[(rows + 8) * 64 :] = jnp.zeros((64, channels), jnp.bfloat16)
    for i in range(rows + 6):
        band = jnp.concatenate(
            [
                jnp.concatenate(
                    [slanted(vecs, i, FORWARD_WIDE + 2 * k + h, mid) for h in range(2)], axis=1
                )
                for k in range(basis_count)
            ],
            axis=0,
        )
        out = dot(band, s0[i * 64 : (i + 4) * 64])
        for k in range(basis_count):
            part = out[k * mid : (k + 1) * mid]
            wide[i * mid : (i + 1) * mid, k * channels : (k + 1) * channels] = part.astype(
                jnp.bfloat16
            )
            if 3 <= i < rows + 3:
                feat0[(i - 3) * cols : (i - 2) * cols, k * channels : (k + 1) * channels] = part[
                    REACH : REACH + cols
                ].astype(jnp.bfloat16)
    pre0[...] = dot(wide[...], weights[0])
    for i in range(rows + 6):
        pre = pre0[i * mid : (i + 1) * mid]
        before = s0[(i + 1) * 64 : (i + 1) * 64 + 3 * cols].astype(jnp.float32)
        before = before[REACH : REACH + mid]
        s1[i * mid : (i + 1) * mid] = (before + pre * jax.nn.sigmoid(pre)).astype(jnp.bfloat16)
    s1[(rows + 6) * mid :] = jnp.zeros((mid, channels), jnp.bfloat16)
    for i in range(rows + 4):
        band = jnp.concatenate(
            [slanted(vecs, i + 1, FORWARD_THIN + k, cols) for k in range(basis_count)], axis=0
        )
        out = dot(band, s1[i * mid : (i + 4) * mid])
        for k in range(basis_count):
            feat1[i * cols : (i + 1) * cols, k * channels : (k + 1) * channels] = out[
                k * cols : (k + 1) * cols
            ].astype(jnp.bfloat16)
    pre1 = dot(feat1[...], weights[1])
    for i in range(rows + 4):
        pre = pre1[i * cols : (i + 1) * cols]
        sigma = jax.nn.sigmoid(pre)
        if 2 <= i < rows + 2:
            before = s1[(i + 1) * mid : (i + 2) * mid].astype(jnp.float32)[REACH : REACH + cols]
            state2[i - 2] = (before + pre * sigma).astype(jnp.bfloat16)
        upstream = cot[i].astype(jnp.float32)[REACH : REACH + cols]
        act1[i] = (upstream * sigma * (1.0 + pre * (1.0 - sigma))).astype(jnp.bfloat16)


def backward_kernel(
    vecs, own, west, east, weights, pre0, cot, act0, grad0, kept, a1, e1, g1, a0, e0
):
    rows, cols, channels = grad0.shape
    basis_count = weights.shape[1] // channels
    mid = cols + 2 * REACH
    full = 3 * cols
    for i in range(rows + 4):
        a1[i * full : i * full + cols] = west[i]
        a1[i * full + cols : i * full + 2 * cols] = own[i]
        a1[i * full + 2 * cols : (i + 1) * full] = east[i]
    for k in range(basis_count):
        errors = dot_nt(a1[...], weights[1, k * channels : (k + 1) * channels])
        errors = errors.astype(jnp.bfloat16)
        for i in range(rows + 4):
            first = (i * basis_count + k) * 64
            e1[first : first + full] = errors[i * full : (i + 1) * full]
            e1[first + full : first + 64] = jnp.zeros((64 - full, channels), jnp.bfloat16)
    parts = []
    for i in range(-2, rows + 2):
        row = i + 2
        band = jnp.concatenate(
            [
                jnp.concatenate(
                    [slanted(vecs, row + 1, BACKWARD_WIDE + 2 * r + h, mid) for h in range(2)],
                    axis=1,
                )
                for r in range(3)
            ],
            axis=0,
        )
        parts.append(dot(band, e1[row * basis_count * 64 : (row + 1) * basis_count * 64]))
        if i < 0:
            continue
        spread = (
            parts[i][2 * mid :] + parts[i + 1][mid : 2 * mid] + parts[i + 2][:mid]
        )
        grad = (cot[i + 1].astype(jnp.float32) + spread).astype(jnp.bfloat16).astype(jnp.float32)
        g1[i * mid : (i + 1) * mid] = grad
        pre = pre0[(i + 2) * mid : (i + 3) * mid]
        sigma = jax.nn.sigmoid(pre)
        act = grad * sigma * (1.0 + pre * (1.0 - sigma))
        a0[i * mid : (i + 1) * mid] = act.astype(jnp.bfloat16)
        if 1 <= i <= rows:
            act0[(i - 1) * cols : i * cols] = act[REACH : REACH + cols].astype(jnp.bfloat16)
    for k in range(basis_count):
        errors = dot_nt(a0[...], weights[0, k * channels : (k + 1) * channels])
        errors = errors.astype(jnp.bfloat16)
        for i in range(rows + 2):
            first = (i * basis_count + k) * mid
            e0[first : first + mid] = errors[i * mid : (i + 1) * mid]
    parts = []
    for i in range(-2, rows):
        row = i + 2
        band = jnp.concatenate(
            [slanted(vecs, row + 2, BACKWARD_THIN + r, cols) for r in range(3)], axis=0
        )
        parts.append(dot(band, e0[row * basis_count * mid : (row + 1) * basis_count * mid]))
        if i < 0:
            continue
        spread = parts[i][2 * cols :] + parts[i + 1][cols : 2 * cols] + parts[i + 2][:cols]
        before = g1[(i + 1) * mid + REACH : (i + 1) * mid + REACH + cols]
        total = (before + spread).astype(jnp.bfloat16)
        grad0[i] = total
        kept[i * cols : (i + 1) * cols] = total


def encoder_kernel(
    owner, taps, field, west, east, cot, masked, partial, down, up, acc
):
    rows_in, cols_in, width = field.shape
    rows, cols, channels = cot.shape
    basis_count = taps.shape[1]
    depth = cols_in + 16
    steps = lax.broadcasted_iota(jnp.int32, (16, width), 0)
    acc[...] = jnp.zeros_like(acc)
    for p in range(rows_in):
        pieces = []
        for k in range(basis_count):
            vector = jnp.broadcast_to(taps[p, k : k + 1], (cols, LANES))
            pieces.append(pltpu.roll(vector, 0, 1, stride=2, stride_axis=0))
        band = jnp.concatenate(pieces, axis=0).astype(jnp.bfloat16)[:, :depth]
        edges = jnp.zeros((16, width), jnp.float32)
        for t in range(TAP_REACH):
            column = slice(t * width, (t + 1) * width)
            edges = jnp.where(steps == t, east[p : p + 1, column].astype(jnp.float32), edges)
            edges = jnp.where(
                steps == 16 - TAP_REACH + t, west[p : p + 1, column].astype(jnp.float32), edges
            )
        out = dot(band, jnp.concatenate([field[p], edges.astype(jnp.bfloat16)], axis=0))
        acc[owner[p]] += out.astype(jnp.bfloat16).astype(jnp.float32)
    for i in range(rows + 2):
        for k in range(basis_count):
            part = acc[i, k * cols : (k + 1) * cols]
            columns = slice(k * width, (k + 1) * width)
            partial[i, :, columns] = part
            if i < 5:
                up[i * cols : (i + 1) * cols, columns] = part.astype(jnp.bfloat16)
            if i >= rows - 3:
                n = i - rows + 3
                down[n * cols : (n + 1) * cols, columns] = part.astype(jnp.bfloat16)
    mid = cols + 2 * REACH
    for message, where, kept in ((down, rows - 2, rows - 8), (up, 0, 0)):
        for n in range(2):
            at = rows_in + (where + n) * REACH
            wide = jnp.concatenate(
                [
                    west[at : at + REACH].astype(jnp.float32),
                    cot[where + n].astype(jnp.float32),
                    east[at : at + REACH].astype(jnp.float32),
                ],
                axis=0,
            )
            message[5 * cols : 5 * cols + mid, n * channels : (n + 1) * channels] = wide.astype(
                jnp.bfloat16
            )
        message[5 * cols + mid :] = jnp.zeros((8, 2 * channels), jnp.bfloat16)
        message[5 * cols + mid :, : masked.shape[1]] = masked[kept : kept + 8]


def in_vmem(count):
    return [pl.BlockSpec(memory_space=pltpu.VMEM)] * count


GRANT = pltpu.CompilerParams(vmem_limit_bytes=26 * 2**20)


def run_encoder(owner, taps, field, west, east, cot, masked):
    rows, cols, channels = cot.shape
    basis_count, width = taps.shape[1], field.shape[2]
    message = jax.ShapeDtypeStruct((5 * cols + cols + 2 * REACH + 8, 2 * channels), jnp.bfloat16)
    return pl.pallas_call(
        encoder_kernel,
        out_shape=(
            jax.ShapeDtypeStruct((rows + 2, cols, basis_count * width), jnp.float32),
            message,
            message,
        ),
        in_specs=[pl.BlockSpec(memory_space=pltpu.SMEM)] + in_vmem(6),
        out_specs=tuple(in_vmem(3)),
        scratch_shapes=[pltpu.VMEM((rows + 2, basis_count * cols, width), jnp.float32)],
        compiler_params=GRANT,
        name="encoder",
    )(owner, taps, field, west, east, cot, masked)


def run_forward(vecs, own, west, east, weights, cot):
    rows, cols, channels = own.shape
    rows -= 8
    depth = weights.shape[1]
    mid = cols + 2 * REACH
    bf16, f32 = jnp.bfloat16, jnp.float32
    return pl.pallas_call(
        forward_kernel,
        out_shape=(
            jax.ShapeDtypeStruct((rows * cols, depth), bf16),
            jax.ShapeDtypeStruct(((rows + 6) * mid, channels), f32),
            jax.ShapeDtypeStruct(((rows + 4) * cols, depth), bf16),
            jax.ShapeDtypeStruct((rows, cols, channels), bf16),
            jax.ShapeDtypeStruct((rows + 4, cols, channels), bf16),
        ),
        in_specs=in_vmem(6),
        out_specs=tuple(in_vmem(5)),
        scratch_shapes=[
            pltpu.VMEM(((rows + 9) * 64, channels), bf16),
            pltpu.VMEM(((rows + 6) * mid, depth), bf16),
            pltpu.VMEM(((rows + 7) * mid, channels), bf16),
        ],
        compiler_params=GRANT,
        name="forward",
    )(vecs, own, west, east, weights, cot)


def run_backward(vecs, own, west, east, weights, pre0, cot):
    rows, cols, channels = own.shape
    rows -= 4
    basis_count = weights.shape[1] // channels
    mid = cols + 2 * REACH
    bf16, f32 = jnp.bfloat16, jnp.float32
    return pl.pallas_call(
        backward_kernel,
        out_shape=(
            jax.ShapeDtypeStruct((rows * cols, channels), bf16),
            jax.ShapeDtypeStruct((rows, cols, channels), bf16),
            jax.ShapeDtypeStruct((rows * cols, channels), bf16),
        ),
        in_specs=in_vmem(7),
        out_specs=tuple(in_vmem(3)),
        scratch_shapes=[
            pltpu.VMEM(((rows + 4) * 3 * cols, channels), bf16),
            pltpu.VMEM(((rows + 4) * basis_count * 64, channels), bf16),
            pltpu.VMEM(((rows + 2) * mid, channels), f32),
            pltpu.VMEM(((rows + 2) * mid, channels), bf16),
            pltpu.VMEM(((rows + 2) * basis_count * mid, channels), bf16),
        ],
        compiler_params=GRANT,
        name="backward",
    )(vecs, own, west, east, weights, pre0, cot)


def per_device(
    input_field,
    encoder_filter,
    row_owner,
    encoder_weight,
    disco_basis,
    row_widths,
    block_weights,
    cotangent,
):
    rows_in, cols_in, in_width = input_field.shape
    rows_dev, cols_dev, channels = cotangent.shape
    basis_count, tap_count = encoder_filter.shape[1:]
    layers = block_weights.shape[0]
    span = disco_basis.shape[3]
    cell_count = rows_dev * cols_dev
    latent_width = basis_count * in_width
    f32, bf16 = jnp.float32, jnp.bfloat16

    def side_message(columns, cot_columns):
        return jnp.concatenate(
            [columns.reshape(rows_in, -1), cot_columns.reshape(-1, channels)]
        )

    west_side = ring_permute(
        side_message(input_field[:, cols_in - TAP_REACH :], cotangent[:, cols_dev - REACH :]),
        "lon",
        1,
    )
    east_side = ring_permute(
        side_message(input_field[:, :TAP_REACH], cotangent[:, :REACH]), "lon", -1
    )
    cot_mid = jnp.concatenate(
        [
            west_side[rows_in:].reshape(rows_dev, REACH, channels),
            cotangent,
            east_side[rows_in:].reshape(rows_dev, REACH, channels),
        ],
        axis=1,
    )
    offsets = jnp.abs(jnp.arange(span, dtype=jnp.int32) - REACH)
    keep = offsets[None, :] <= row_widths[:, None]
    masked = jnp.where(keep[:, None, None, :], disco_basis, jnp.zeros_like(disco_basis))
    masked = masked.reshape(rows_dev, -1)
    first_row = lax.axis_index(BAND) * rows_dev - 1
    tap_lanes = np.zeros((tap_count, LANES), np.float32)
    for t in range(tap_count):
        tap_lanes[t, (t - TAP_REACH) % LANES] = 1
        if t < TAP_REACH:
            tap_lanes[t, cols_in + 16 - TAP_REACH + t] = 1
    taps = jnp.einsum(
        "pkt,tl->pkl", encoder_filter, jnp.asarray(tap_lanes, bf16), preferred_element_type=f32
    )
    partial, down, up = run_encoder(
        row_owner - first_row, taps, input_field, west_side, east_side, cotangent, masked
    )
    above = line_permute(down, BAND, 1)
    below = line_permute(up, BAND, -1)
    lat_rows = 5 * cols_dev

    def opened(message, kept):
        latent = message[:lat_rows].reshape(5, cols_dev, latent_width).astype(f32)
        cot = message[lat_rows:-8]
        cot = jnp.stack([cot[:, :channels], cot[:, channels:]])
        return latent, cot, message[-8:][kept, : masked.shape[1]]

    above_latent, above_cot, above_basis = opened(above, slice(5, 8))
    below_latent, below_cot, below_basis = opened(below, slice(0, 3))
    tail = rows_dev + 3
    latent = (
        jnp.pad(partial, ((3, 3), (0, 0), (0, 0)))
        + jnp.pad(above_latent, ((0, tail), (0, 0), (0, 0)))
        + jnp.pad(below_latent, ((tail, 0), (0, 0), (0, 0)))
    ).astype(bf16)
    state0 = jnp.dot(
        latent.reshape(-1, latent_width), encoder_weight, preferred_element_type=f32
    ).astype(bf16)
    state0 = state0.reshape(rows_dev + 8, cols_dev, channels)
    west = ring_permute(state0, "lon", 1)
    east = ring_permute(state0, "lon", -1)
    cot_ext = jnp.concatenate([above_cot, cot_mid, below_cot])
    basis_ext = jnp.concatenate([above_basis, masked, below_basis])
    vecs = jnp.dot(
        basis_ext, jnp.asarray(placement(basis_count, span), bf16), preferred_element_type=f32
    )
    feat0, pre0, feat1, state_out, act1 = run_forward(
        vecs, state0, west, east, block_weights, cot_ext
    )

    act_west = ring_permute(act1, "lon", 1)
    act_east = ring_permute(act1, "lon", -1)
    inner = slice(2 * cols_dev, 2 * cols_dev + cell_count)
    weight1 = lax.dot_general(
        feat1[inner],
        act1.reshape(-1, channels)[inner],
        (((0,), (0,)), ((), ())),
        preferred_element_type=f32,
    )
    act0, gradient, gradient_rows = run_backward(
        vecs, act1, act_west, act_east, block_weights, pre0, cot_ext
    )
    weight0 = lax.dot_general(
        feat0, act0, (((0,), (0,)), ((), ())), preferred_element_type=f32
    )
    encoder_term = lax.dot_general(
        latent[4 : rows_dev + 4].reshape(cell_count, latent_width),
        gradient_rows,
        (((0,), (0,)), ((), ())),
        preferred_element_type=f32,
    )
    grads = jnp.concatenate([weight0, weight1, encoder_term], axis=0).astype(bf16)
    grad_sum = sum_over_cells(grads)
    block_rows = layers * basis_count * channels
    cells_total = cell_count * lax.axis_size("lon") * lax.axis_size(BAND)
    normalizer = 1.0 / math.sqrt(cells_total)
    block_grads = (grad_sum[:block_rows] * normalizer).reshape(
        layers, basis_count * channels, grad_sum.shape[1]
    )
    return (state_out, gradient, block_grads, grad_sum[block_rows:] * normalizer)


def solution(mesh):
    placed = (
        P(("ens", "lat", "ch"), "lon", None),
        P(("lat", "ch"), None, None),
        P(("ens", "lat", "ch")),
        P(),
        P(("lat", "ch"), None, None, None),
        P(("lat", "ch")),
        P(),
        P(("ens", "lat", "ch"), "lon", None),
    )
    return jax.shard_map(
        per_device,
        mesh=mesh,
        in_specs=placed,
        out_specs=(
            P(("ens", "lat", "ch"), "lon", None),
            P(("ens", "lat", "ch"), "lon", None),
            P("ens", None, "ch"),
            P("ens", "ch"),
        ),
        check_vma=False,
    )
```
